256 devices in a mesh: dp: 32 (over y, z), tensor: 8 (over x, core).
Axes of the slice: x: 4, y: 4, z: 8, core: 2. Of those that a mesh axis runs over, the one named last changes fastest.
Arguments:
- qkv: bfloat16 [3, 16384, 4096], P(None, 'dp', 'tensor'), may hold values from -6 to 6
- segment_ids: int32 [32, 8, 64], P('dp'), may hold values from 0 to 1, never falling along the last dimension, each value on 1 to 63 neighbouring positions
- out_weight: bfloat16 [4096, 4096], P(None, 'tensor'), may hold values from -0.09375 to 0.09375
- out_bias: bfloat16 [4096], replicated, may hold values from -3 to 3
- upstream: bfloat16 [16384, 4096], P(('dp', 'tensor')), may hold values from -24 to 24
- pre_act: bfloat16 [16384, 8192], P('dp', 'tensor'), may hold values from -6 to 6
- down_weight: bfloat16 [4096, 8192], P('dp', 'tensor'), may hold values from -0.0625 to 0.0625
Outputs:
- attention_out: float32 [16384, 4096], P(('dp', 'tensor'))
- act_grad: float32 [16384, 8192], P('dp', 'tensor')
- weight_grad: float32 [4096, 8192], P('dp', 'tensor')
The draws below stay inside these ranges and needn't reach their ends.
Inputs may be any that keep to these rules, and one draw needn't show every extreme that they name: `segment_ids`: within each pack the ids never fall; 2 images a pack, each of 1 to 63 tokens.
All inputs are finite; a program needn't handle non-finite values.
Results may differ from the reference program's by a relative error of at most 0.0055.
Values may be sent and summed in bfloat16 or wider, within the bound.
A program may use at most 128 MiB of HBM per device.

```python
import math
import jax
import jax.numpy as jnp
import numpy as np
from jax import lax

D = 4096
HEADS = 32
HEAD = 128
FF = 8192
ROWS_DEV = 64
TOKENS = 512
BATCH = 16384
HD = 4096
IMG_PACK = 2
MOST_IMG = 63
N_DP = 32
N_TENSOR = 8


def draw_qkv(key, part):
    sample = jax.random.truncated_normal(key, -6.0, 6.0, (3, BATCH, HD), jnp.float32)
    return sample.astype(jnp.bfloat16)


def spiked(result, key, source, target, shards_of, factor):
    def block_of(dim):
        return (jnp.arange(result.shape[dim]) // (result.shape[dim] // shards_of)).reshape((-1,) + (1,) * (result.ndim - 1 - dim))

    near = jax.random.permutation(key, shards_of)[block_of(target)]
    far = (block_of(target) + shards_of // 2) % shards_of
    return jnp.where((block_of(source) == near) | (block_of(source) == far), factor * result, result)


def shard_levels(stream_key, extent, pieces, least, largest):
    loudness = 1.0
    for dim, parts in pieces:
        steps = jax.random.uniform(jax.random.fold_in(jax.random.fold_in(stream_key, 6), dim), (parts,), jnp.float32, least / len(pieces), largest / len(pieces))
        loudness = loudness * jnp.repeat(jnp.exp(steps), extent[dim] // parts).reshape((-1,) + (1,) * (len(extent) - 1 - dim))
    return loudness


def profile(number_of, total, limit, lean):
    weights = [(1 << 20) // math.isqrt(rank ** lean) + 1 for rank in range(2, number_of + 1)]
    surplus, given = total - limit - (number_of - 1), [1] * (number_of - 1)
    while surplus > 0:
        movable = [i for i in range(number_of - 1) if given[i] < limit]
        mass, remaining = sum([weights[i] for i in movable]), surplus
        for i in movable:
            addition = min(limit - given[i], max(1, remaining * weights[i] // mass), surplus)
            given[i] = given[i] + addition
            surplus = surplus - addition
    return np.array([limit] + given)


def uneven(stream_key, number_of, total, most, lean):
    if number_of == 2:
        one = jax.random.randint(stream_key, (), max(1, total - most), min(most, total - 1) + 1)
        return jnp.stack([one, total - one])
    lengths = jnp.asarray(profile(number_of, total, most, lean), jnp.int32)
    pairs = (number_of - 1) // 2
    donor, receiver = lengths[1:1 + 2 * pairs:2], lengths[2:2 + 2 * pairs:2]
    slack = jnp.minimum(donor - 1, most - receiver)
    passed = jax.random.randint(jax.random.fold_in(stream_key, 1), (pairs,), 0, 1 << 20) % (slack + 1)
    lengths = lengths.at[1:1 + 2 * pairs:2].set(donor - passed).at[2:2 + 2 * pairs:2].set(receiver + passed)
    return lengths[jax.random.permutation(jax.random.fold_in(stream_key, 2), number_of)]


def normal_values(own_key, dims, deviation, most, shards=(), kind=jnp.bfloat16):
    result = deviation * jax.random.normal(own_key, dims, jnp.float32)
    if shards:
        result = result * shard_levels(own_key, dims, shards, -0.22, 0.18)
    return jnp.clip(result, -most, most).astype(kind)


def noise_with(key, extent, spread, most, shards, heavy, kind=jnp.bfloat16):
    values = spread * jax.random.normal(key, extent, jnp.float32)
    if shards:
        values = values * shard_levels(key, extent, shards, -0.22, 0.18)
    return jnp.clip(spiked(values, jax.random.fold_in(key, 3), *heavy), -most, most).astype(kind)


def setup_inputs(seed: int = 0) -> dict:
    splits = jax.random.split(jax.random.key(seed), 8)
    return {
        "qkv": draw_qkv(jax.random.fold_in(splits[7], 71), 0),
        "segment_ids": jax.vmap(lambda own: jnp.searchsorted(jnp.cumsum(uneven(own, IMG_PACK, ROWS_DEV, MOST_IMG, 2)), jnp.arange(ROWS_DEV), side="right"))(jax.random.split(splits[1], N_DP * N_TENSOR)).reshape((N_DP, N_TENSOR, ROWS_DEV)).astype(jnp.int32),
        "out_weight": normal_values(splits[2], (D, HD), HD ** -0.5, 0.09375, ((1, 8),)),
        "out_bias": normal_values(splits[3], (D,), 0.5, 3.0),
        "upstream": noise_with(splits[4], (BATCH, D), 1.0, 24.0, ((0, 256),), (0, 1, 256, 6.0)),
        "pre_act": normal_values(splits[5], (BATCH, FF), 1.0, 6.0, ((0, 32), (1, 8))),
        "down_weight": normal_values(splits[6], (D, FF), FF ** -0.5, 0.0625, ((0, 32), (1, 8))),
    }


root_half = 1.0 / math.sqrt(2.0)
inv_root_tau = 1.0 / math.sqrt(2.0 * math.pi)

def gelu_exact(argument):
    return 0.5 * argument * (1.0 + lax.erf(argument * root_half))

def gelu_slope(argument):
    return 0.5 * (1.0 + lax.erf(argument * root_half)) + argument * jnp.exp(-0.5 * argument * argument) * inv_root_tau

def attend(bundle):
    queries, key_rows, value_rows, labels = bundle
    length = queries.shape[0]
    queries = queries.reshape(length, HEADS, HEAD).astype(jnp.float32)
    key_rows = key_rows.reshape(length, HEADS, HEAD).astype(jnp.float32)
    value_rows = value_rows.reshape(length, HEADS, HEAD).astype(jnp.float32)
    scores = jnp.einsum('qhd,khd->hqk', queries, key_rows) * (1.0 / math.sqrt(HEAD))
    pack_of = jnp.arange(length, dtype=jnp.int32) // ROWS_DEV
    same_image = ((labels[:, None] == labels[None, :]) & (pack_of[:, None] == pack_of[None, :]))[None]
    masked = jnp.where(same_image, scores, -1e+30)
    row_top = lax.optimization_barrier(jnp.max(masked, axis=2, keepdims=True))
    exponent = jnp.where(same_image, jnp.exp(masked - row_top), 0.0)
    weights = (exponent / lax.optimization_barrier(jnp.sum(exponent, axis=2, keepdims=True))).astype(jnp.bfloat16)
    context = jnp.einsum('hqk,khd->qhd', weights.astype(jnp.float32), value_rows)
    return context.reshape(length, HD).astype(jnp.bfloat16)

def reference(qkv, segment_ids, out_weight, out_bias, upstream, pre_act, down_weight):
    packed = qkv.reshape(3, N_DP, TOKENS, HD)
    labels = segment_ids.reshape(N_DP, TOKENS)
    context = lax.map(attend, (packed[0], packed[1], packed[2], labels))
    context = context.reshape(BATCH, HD)
    share = HD // N_TENSOR
    running = jnp.zeros((BATCH, D), jnp.float32)
    for member in range(N_TENSOR):
        ctx_part = context[:, member * share:(member + 1) * share]
        weight_part = out_weight[:, member * share:(member + 1) * share]
        partial_value = lax.dot_general(ctx_part, weight_part, (((1,), (1,)), ((), ())), preferred_element_type=jnp.float32)
        rounded = lax.optimization_barrier(partial_value.astype(jnp.bfloat16))
        running = running + rounded.astype(jnp.float32)
    attention_out = running + out_bias.astype(jnp.float32)
    hidden_grad = jnp.dot(upstream, down_weight, preferred_element_type=jnp.float32)
    preact = pre_act.astype(jnp.float32)
    act_grad = hidden_grad * gelu_slope(preact)
    activation = gelu_exact(preact).astype(jnp.bfloat16)
    weight_grad = lax.dot_general(upstream, activation, (((0,), (0,)), ((), ())), preferred_element_type=jnp.float32) / N_DP
    return (attention_out, act_grad, weight_grad)
```

```python
import functools
import math

import jax
import jax.numpy as jnp
from jax import lax
from jax.experimental import pallas as pl
from jax.experimental.pallas import tpu as pltpu
from jax.sharding import Mesh
from jax.sharding import PartitionSpec as P

HEAD = 128
DP = ("y", "z")
DP_TENSOR = ("y", "z", "x", "c")
BF = jnp.bfloat16
F32 = jnp.float32

ROOT_HALF = 1.0 / math.sqrt(2.0)
INV_ROOT_TAU = 1.0 / math.sqrt(2.0 * math.pi)
SCALE = 1.0 / math.sqrt(HEAD)


class Ids:
    def __init__(self):
        self.n = 0

    def take(self, count=1):
        first = self.n
        self.n += count
        return first


IDS = Ids()
U1 = IDS.take(4)
U2R, U2L = IDS.take(4), IDS.take(4)
U2FR, U2FL = IDS.take(4), IDS.take(4)
U2S = IDS.take(4)
WR, WL = IDS.take(4), IDS.take(4)
AR, AL = IDS.take(4), IDS.take(4)
ARF, ALF = IDS.take(4), IDS.take(4)
ATS = IDS.take(4)
ATH, ATF = IDS.take(2), IDS.take(2)
HHS, HFS = IDS.take(2), IDS.take(4)
GRS = IDS.take(16)
N_IDS = IDS.n

LOCAL = Ids()
L_QKV, L_SEG, L_OW, L_PRE, L_UP, L_W, L_BIAS = (LOCAL.take() for _ in range(7))
L_ATT, L_WG = LOCAL.take(), LOCAL.take()
L_ACT = LOCAL.take(4)
N_LOCAL = LOCAL.n


def kernel(
    qkv, seg, out_weight, bias, upstream, pre_act, down_weight,
    att_hbm, act_hbm, wg_hbm,
    qkv_v, seg_v, ow_v, bias_v, pre_v, slope_v, ug, wg, ag, ctx,
    att_p, att_r, att_h, att_f, att_o,
    hp, hh, hf, h0, acc, gs, gr, go,
    ssem, rsem, lsem,
):
    y, z, x, c = (lax.axis_index(name) for name in ("y", "z", "x", "c"))
    t = 2 * x + c
    yy = [lax.rem(y + d, 4) for d in range(4)]
    zz = [lax.rem(z + d, 8) for d in range(8)]
    xx = [lax.rem(x + d, 4) for d in range(4)]
    oc = 1 - c
    sent = []
    local = []

    def send(k, src, dst, **where):
        copy = pltpu.make_async_remote_copy(
            src_ref=src, dst_ref=dst, send_sem=ssem.at[k], recv_sem=rsem.at[k],
            device_id=where, device_id_type=pl.DeviceIdType.MESH,
        )
        copy.start()
        sent.append(copy)

    def arrived(k, dst, **where):
        pltpu.make_async_remote_copy(
            src_ref=dst, dst_ref=dst, send_sem=ssem.at[k], recv_sem=rsem.at[k],
            device_id=where, device_id_type=pl.DeviceIdType.MESH,
        ).wait_recv()

    def fetch(k, src, dst):
        copy = pltpu.make_async_copy(src, dst, lsem.at[k])
        copy.start()
        return copy

    got_pre = fetch(L_PRE, pre_act, pre_v)
    got_up = fetch(L_UP, upstream.at[:, pl.ds(pl.multiple_of(y * 1024, 1024), 1024)], ug.at[y, t])
    got_w = fetch(L_W, down_weight, wg.at[z])
    got_seg = fetch(L_SEG, seg, seg_v)
    got_qkv = fetch(L_QKV, qkv, qkv_v)
    got_bias = fetch(L_BIAS, bias, bias_v)
    got_ow = fetch(L_OW, out_weight, ow_v)

    barrier = pltpu.get_barrier_semaphore()
    peers = [{"y": yy[d]} for d in (1, 2, 3)] + [{"z": zz[d]} for d in (1, 7)]
    peers += [{"x": xx[d]} for d in (1, 3)] + [{"c": oc}]
    for peer in peers:
        pl.semaphore_signal(barrier, inc=1, device_id=peer, device_id_type=pl.DeviceIdType.MESH)
    pl.semaphore_wait(barrier, len(peers))

    got_w.wait()
    send(WR, wg.at[z], wg.at[z], z=zz[1])
    send(WL, wg.at[z], wg.at[z], z=zz[7])
    for d in (1, 3, 2):
        columns = pl.ds(pl.multiple_of(yy[d] * 1024, 1024), 1024)
        send(U1 + d, upstream.at[:, columns], ug.at[y, t], y=yy[d])
    got_up.wait()
    send(U2R, ug.at[y, t], ug.at[y, t], x=xx[1])
    send(U2L, ug.at[y, t], ug.at[y, t], x=xx[3])

    got_pre.wait()

    def gelu(q):
        def rows(i, carry):
            here = pl.ds(pl.multiple_of(q * 128 + i * 16, 16), 16)
            v = pre_v[here, :].astype(F32)
            tail = 1.0 + lax.erf(v * ROOT_HALF)
            ag[y, here, :] = (0.5 * v * tail).astype(BF)
            slope_v[here, :] = 0.5 * tail + v * jnp.exp(-0.5 * v * v) * INV_ROOT_TAU
            return carry

        lax.fori_loop(0, 8, rows, 0)
        part = pl.ds(q * 128, 128)
        send(AR + q, ag.at[y, part], ag.at[y, part], y=yy[1])
        send(AL + q, ag.at[y, part], ag.at[y, part], y=yy[3])

    def own_upstream(e):
        arrived(U1 + (4 - e), ug.at[yy[e], t], y=yy[e])
        send(U2R + e, ug.at[yy[e], t], ug.at[yy[e], t], x=xx[1])
        send(U2L + e, ug.at[yy[e], t], ug.at[yy[e], t], x=xx[3])

    t_left, t_right, t_far = 2 * xx[3] + c, 2 * xx[1] + c, 2 * xx[2] + c

    def upstream_from_left(e, forward):
        slot = ug.at[yy[e], t_left]
        arrived(U2R + e, slot, x=xx[3])
        if forward:
            send(U2FR + e, slot, slot, x=xx[1])

    def upstream_from_right(e, forward):
        slot = ug.at[yy[e], t_right]
        arrived(U2L + e, slot, x=xx[1])
        if forward:
            send(U2FL + e, slot, slot, x=xx[3])

    def weight_hop(s):
        from_left, from_right = zz[8 - s], zz[s]
        arrived(WR + s - 1, wg.at[from_left], z=zz[7])
        arrived(WL + s - 1, wg.at[from_right], z=zz[1])
        if s < 3:
            send(WR + s, wg.at[from_left], wg.at[from_left], z=zz[1])
            send(WL + s, wg.at[from_right], wg.at[from_right], z=zz[7])
        else:
            low, high = pl.ds(0, 64), pl.ds(64, 64)
            send(WR + s, wg.at[from_left, low], wg.at[from_left, low], z=zz[1])
            send(WL + s, wg.at[from_right, high], wg.at[from_right, high], z=zz[7])

    def act_from_left(q, forward):
        slot = ag.at[yy[3], pl.ds(q * 128, 128)]
        arrived(AR + q, slot, y=yy[3])
        if forward:
            send(ARF + q, slot, slot, y=yy[1])

    def act_from_right(q, forward):
        slot = ag.at[yy[1], pl.ds(q * 128, 128)]
        arrived(AL + q, slot, y=yy[1])
        if forward:
            send(ALF + q, slot, slot, y=yy[3])

    gelu(0)
    gelu(1)
    own_upstream(3)
    own_upstream(1)
    gelu(2)
    gelu(3)
    own_upstream(2)
    send(U2S, ug.at[:, t], ug.at[:, t], c=oc)
    weight_hop(1)

    got_seg.wait()
    got_qkv.wait()
    labels = seg_v[0].astype(F32)
    row_i = lax.broadcasted_iota(jnp.int32, (128, 1), 0)
    col_i = lax.broadcasted_iota(jnp.int32, (1, 128), 1)
    for pair in range(4):
        first = [
            (64.0 - jnp.sum(labels[2 * pair + p : 2 * pair + p + 1, :], axis=1, keepdims=True)).astype(jnp.int32)
            for p in range(2)
        ]

        def image(i):
            second_pack = i >= 64
            place = jnp.where(second_pack, i - 64, i)
            bound = jnp.where(second_pack, first[1], first[0])
            return jnp.where(second_pack, 2, 0) + jnp.where(place >= bound, 1, 0)

        same = image(row_i) == image(col_i)
        rows = pl.ds(pair * 128, 128)
        for h in range(4):
            cols = pl.ds(h * 128, 128)
            s = lax.dot_general(
                qkv_v[0, rows, cols], qkv_v[1, rows, cols], (((1,), (1,)), ((), ())),
                preferred_element_type=F32,
            ) * SCALE
            s = jnp.where(same, s, -1e30)
            e = jnp.where(same, jnp.exp(s - jnp.max(s, axis=1, keepdims=True)), 0.0)
            w = (e / jnp.sum(e, axis=1, keepdims=True)).astype(BF)
            ctx[rows, cols] = jnp.dot(w, qkv_v[2, rows, cols], preferred_element_type=F32).astype(BF)

    upstream_from_left(0, True)
    upstream_from_right(3, True)
    act_from_left(0, True)
    got_ow.wait()

    def project(n, carry):
        cols = pl.ds(pl.multiple_of(n * 512, 512), 512)
        part = lax.dot_general(
            ctx[...], ow_v[cols, :], (((1,), (1,)), ((), ())), preferred_element_type=F32
        )
        att_p[:, :, :, cols] = part.astype(BF).reshape(4, 2, 64, 512)
        return carry

    lax.fori_loop(0, 4, project, 0)
    weight_hop(2)
    act_from_left(1, True)
    lax.fori_loop(4, 8, project, 0)
    order = (2, 1, 3, 0)
    for e in order:
        send(ATS + e, att_p.at[xx[e], oc], att_r.at[xx[e]], c=oc)
    upstream_from_left(1, True)
    upstream_from_right(2, True)
    for e in (2, 3):
        upstream_from_left(e, False)
    for e in (0, 1):
        upstream_from_right(e, False)
    send(U2S + 1, ug.at[:, t_left], ug.at[:, t_left], c=oc)
    send(U2S + 2, ug.at[:, t_right], ug.at[:, t_right], c=oc)
    act_from_right(2, True)

    def chip_sum(e):
        arrived(ATS + e, att_r.at[xx[e]], c=oc)

        def rows(i, carry):
            here = pl.ds(pl.multiple_of(i * 16, 16), 16)
            both = att_p[xx[e], c, here, :].astype(F32) + att_r[xx[e], here, :].astype(F32)
            att_p[xx[e], c, here, :] = both.astype(BF)
            return carry

        lax.fori_loop(0, 4, rows, 0)

    chip_sum(2)
    for k, cols in enumerate((pl.ds(0, 2048), pl.ds(2048, 2048))):
        send(ATH + k, att_p.at[xx[2], c, :, cols], att_h.at[k], x=xx[1] if k == 0 else xx[3])
    weight_hop(3)
    act_from_right(3, True)
    for e in (1, 3):
        chip_sum(e)

    for e in (0, 1):
        arrived(U2FR + e, ug.at[yy[e], t_far], x=xx[3])
    for e in (3, 2):
        arrived(U2FL + e, ug.at[yy[e], t_far], x=xx[1])
    send(U2S + 3, ug.at[:, t_far], ug.at[:, t_far], c=oc)
    for k, dx in ((0, 0), (1, 3), (2, 1), (3, 2)):
        arrived(U2S + k, ug.at[:, 2 * xx[dx] + oc], c=oc)
    low, high = pl.ds(0, 64), pl.ds(64, 64)
    arrived(WR + 3, wg.at[zz[4], low], z=zz[7])
    arrived(WL + 3, wg.at[zz[4], high], z=zz[1])

    def hidden(d, store):
        def tile(n, carry):
            cols = pl.ds(pl.multiple_of(n * 256, 256), 256)
            store(
                cols,
                jnp.dot(
                    ug[yy[d]].reshape(512, 1024), wg[:, :, cols].reshape(1024, 256),
                    preferred_element_type=F32,
                ),
            )
            return carry

        lax.fori_loop(0, 4, tile, 0)

    def to_send(d):
        def store(cols, value):
            hp[d - 1, :, cols] = value.astype(BF)

        return store

    def to_keep(cols, value):
        h0[:, cols] = value

    top, bottom = pl.ds(0, 256), pl.ds(256, 256)
    hidden(2, to_send(2))
    send(HHS, hp.at[1, top], hh.at[0], y=yy[1])
    send(HHS + 1, hp.at[1, bottom], hh.at[1], y=yy[3])
    hidden(1, to_send(1))
    send(HFS, hp.at[0, bottom], hf.at[0, bottom], y=yy[1])
    hidden(3, to_send(3))
    send(HFS + 1, hp.at[2, top], hf.at[1, top], y=yy[3])

    for k, e, lo in ((0, 1, 0), (1, 3, 2048)):
        arrived(ATH + k, att_h.at[k], x=xx[3] if k == 0 else xx[1])

        def add_half(i, carry, k=k, e=e, lo=lo):
            here = pl.ds(pl.multiple_of(i * 16, 16), 16)
            cols = pl.ds(lo, 2048)
            total = att_p[xx[e], c, here, cols].astype(F32) + att_h[k, here, :].astype(F32)
            att_p[xx[e], c, here, cols] = total.astype(BF)
            return carry

        lax.fori_loop(0, 4, add_half, 0)
        send(ATF + k, att_p.at[xx[e], c], att_f.at[k], x=xx[e])

    hidden(0, to_keep)

    def weight_part(e, first):
        def tile(m, carry):
            cols = pl.ds(pl.multiple_of(m * 256, 256), 256)
            part = lax.dot_general(
                ug[yy[e], :, :, cols].reshape(512, 256), ag[yy[e]], (((0,), (0,)), ((), ())),
                preferred_element_type=F32,
            ).reshape(2, 128, 1024)
            here = pl.ds(2 * m, 2)
            if first:
                acc[here] = part
            else:
                acc[here] = acc[here] + part
            return carry

        lax.fori_loop(0, 4, tile, 0)

    weight_part(0, True)
    for q in (2, 3):
        act_from_left(q, False)
    weight_part(3, False)
    for q in (0, 1):
        act_from_right(q, False)
    weight_part(1, False)
    for q in (0, 1):
        arrived(ARF + q, ag.at[yy[2], pl.ds(q * 128, 128)], y=yy[3])
    for q in (2, 3):
        arrived(ALF + q, ag.at[yy[2], pl.ds(q * 128, 128)], y=yy[1])
    weight_part(2, False)

    def grad_id(k, s, half):
        return GRS + (k * 4 + s) * 2 + half

    def grad_send(k, s, half, add):
        target = zz[4 - s] if k == 0 else zz[4 + s]
        here = pl.ds(half * 64, 64)
        came = zz[7] if k == 0 else zz[1]
        if add:
            arrived(grad_id(k, s - 1, half), gr.at[k, s - 1, here], z=came)
            gs[k, s, here, :] = (acc[target, here, :] + gr[k, s - 1, here, :].astype(F32)).astype(BF)
        else:
            gs[k, s, here, :] = acc[target, here, :].astype(BF)
        send(grad_id(k, s, half), gs.at[k, s, here], gr.at[k, s, here], z=zz[1] if k == 0 else zz[7])

    grad_send(0, 0, 0, False)
    grad_send(1, 0, 1, False)
    grad_send(0, 1, 1, False)
    grad_send(1, 1, 0, False)

    arrived(ATS, att_r.at[x], c=oc)
    for k in range(2):
        arrived(ATF + k, att_f.at[k], x=xx[3] if k == 0 else xx[1])
    got_bias.wait()

    def att_rows(i, carry):
        here = pl.ds(pl.multiple_of(i * 16, 16), 16)
        total = att_p[x, c, here, :].astype(F32) + att_r[x, here, :].astype(F32)
        total = total + att_f[0, here, :].astype(F32) + att_f[1, here, :].astype(F32)
        att_o[here, :] = total + bias_v[...].astype(F32)
        return carry

    lax.fori_loop(0, 4, att_rows, 0)
    local.append(fetch(L_ATT, att_o, att_hbm))

    grad_send(0, 1, 0, True)
    grad_send(1, 1, 1, True)
    grad_send(0, 2, 1, True)
    grad_send(1, 2, 0, True)

    def hidden_hop(k):
        slot, here = (0, top) if k == 0 else (2, bottom)
        arrived(HHS + k, hh.at[k], y=yy[3] if k == 0 else yy[1])
        start = 0 if k == 0 else 256

        def rows(i, carry):
            there = pl.ds(pl.multiple_of(i * 16, 16), 16)
            mine = pl.ds(pl.multiple_of(start + i * 16, 16), 16)
            total = hp[slot, mine, :].astype(F32) + hh[k, there, :].astype(F32)
            hp[slot, mine, :] = total.astype(BF)
            return carry

        lax.fori_loop(0, 16, rows, 0)
        send(HFS + 2 + k, hp.at[slot, here], hf.at[k, here], y=yy[1] if k == 0 else yy[3])

    hidden_hop(0)
    hidden_hop(1)
    for s, halves in ((2, (0, 1)), (3, (1, 0)), (3, (0, 1))):
        grad_send(0, s, halves[0], True)
        grad_send(1, s, halves[1], True)

    arrived(HFS, hf.at[0, bottom], y=yy[3])
    arrived(HFS + 1, hf.at[1, top], y=yy[1])

    def fold(k, start):
        def rows(i, carry):
            here = pl.ds(pl.multiple_of(start + i * 16, 16), 16)
            h0[here, :] = h0[here, :] + hf[k, here, :].astype(F32)
            return carry

        lax.fori_loop(0, 16, rows, 0)

    fold(0, 256)
    fold(1, 0)

    for half in (0, 1):
        here = pl.ds(half * 64, 64)
        for k in range(2):
            arrived(grad_id(k, 3, half), gr.at[k, 3, here], z=zz[7] if k == 0 else zz[1])
        total = acc[z, here, :] + gr[0, 3, here, :].astype(F32) + gr[1, 3, here, :].astype(F32)
        go[here, :] = total * (1.0 / 32.0)
    local.append(fetch(L_WG, go, wg_hbm))

    def finish(k, start):
        def rows(i, carry):
            here = pl.ds(pl.multiple_of(start + i * 16, 16), 16)
            h0[here, :] = (h0[here, :] + hf[k, here, :].astype(F32)) * slope_v[here, :]
            return carry

        lax.fori_loop(0, 16, rows, 0)
        part = pl.ds(start, 256)
        local.append(fetch(L_ACT + k, h0.at[part], act_hbm.at[part]))

    arrived(HFS + 2, hf.at[0, top], y=yy[3])
    finish(0, 0)
    arrived(HFS + 3, hf.at[1, bottom], y=yy[1])
    finish(1, 256)

    for copy in sent:
        copy.wait_send()
    for copy in local:
        copy.wait()


def body(qkv, segment_ids, out_weight, out_bias, upstream, pre_act, down_weight):
    hbm = pl.BlockSpec(memory_space=pl.ANY)
    vmem = pltpu.VMEM
    return pl.pallas_call(
        kernel,
        out_shape=(
            jax.ShapeDtypeStruct((64, 4096), F32),
            jax.ShapeDtypeStruct((512, 1024), F32),
            jax.ShapeDtypeStruct((128, 1024), F32),
        ),
        in_specs=[hbm] * 7,
        out_specs=(hbm,) * 3,
        scratch_shapes=[
            vmem((3, 512, 512), BF),
            vmem((1, 8, 64), jnp.int32),
            vmem((4096, 512), BF),
            vmem((1, 4096), BF),
            vmem((512, 1024), BF),
            vmem((512, 1024), F32),
            vmem((4, 8, 64, 1024), BF),
            vmem((8, 128, 1024), BF),
            vmem((4, 512, 1024), BF),
            vmem((512, 512), BF),
            vmem((4, 2, 64, 4096), BF),
            vmem((4, 64, 4096), BF),
            vmem((2, 64, 2048), BF),
            vmem((2, 64, 4096), BF),
            vmem((64, 4096), F32),
            vmem((3, 512, 1024), BF),
            vmem((2, 256, 1024), BF),
            vmem((2, 512, 1024), BF),
            vmem((512, 1024), F32),
            vmem((8, 128, 1024), F32),
            vmem((2, 4, 128, 1024), BF),
            vmem((2, 4, 128, 1024), BF),
            vmem((128, 1024), F32),
            pltpu.SemaphoreType.DMA((N_IDS,)),
            pltpu.SemaphoreType.DMA((N_IDS,)),
            pltpu.SemaphoreType.DMA((N_LOCAL,)),
        ],
        compiler_params=pltpu.CompilerParams(
            collective_id=0, has_side_effects=True, vmem_limit_bytes=63 * 1024 * 1024
        ),
        name="layer",
    )(qkv, segment_ids, out_weight, out_bias.reshape(1, -1), upstream, pre_act, down_weight)


def solution(mesh):
    finer = Mesh(mesh.devices.reshape(4, 8, 4, 2), ("y", "z", "x", "c"))
    tensor = ("x", "c")
    in_specs = (
        P(None, DP, tensor),
        P(DP, None, None),
        P(None, tensor),
        P(),
        P(DP_TENSOR, None),
        P(DP, tensor),
        P(DP, tensor),
    )
    out_specs = (P(DP_TENSOR, None), P(DP, tensor), P(DP, tensor))
    return jax.shard_map(body, mesh=finer, in_specs=in_specs, out_specs=out_specs, check_vma=False)
```

```python
import math

import jax
import jax.numpy as jnp
from jax import lax
from jax.experimental import pallas as pl
from jax.experimental.pallas import tpu as pltpu
from jax.sharding import Mesh
from jax.sharding import PartitionSpec as P

HEAD = 128
DP = ("y", "z")
DP_TENSOR = ("y", "z", "x", "c")
BF = jnp.bfloat16
F32 = jnp.float32

ROOT_HALF = 1.0 / math.sqrt(2.0)
INV_ROOT_TAU = 1.0 / math.sqrt(2.0 * math.pi)
SCALE = 1.0 / math.sqrt(HEAD)


class Ids:
    def __init__(self):
        self.n = 0

    def take(self, count=1):
        first = self.n
        self.n += count
        return first


IDS = Ids()
U1 = IDS.take(4)
U2R, U2L = IDS.take(4), IDS.take(4)
U2FR, U2FL = IDS.take(4), IDS.take(4)
U2S = IDS.take(4)
UOR, UOL = IDS.take(4), IDS.take(4)
UOFR, UOFL = IDS.take(4), IDS.take(4)
UOS = IDS.take(4)
WY = IDS.take(4)
WR, WL = IDS.take(4), IDS.take(4)
WOR, WOL = IDS.take(4), IDS.take(4)
AR, AL = IDS.take(4), IDS.take(4)
ARF, ALF = IDS.take(4), IDS.take(4)
ATS = IDS.take(4)
ATH, ATF = IDS.take(2), IDS.take(2)
HHS, HFS = IDS.take(2), IDS.take(4)
GRS = IDS.take(16)
N_IDS = IDS.n

LOCAL = Ids()
L_QKV, L_SEG, L_OW, L_PRE, L_UP, L_W, L_BIAS = (LOCAL.take() for _ in range(7))
L_UO = LOCAL.take(4)
N_LOCAL = LOCAL.n

CO = 256
CQ = 1024 - CO


def kernel(
    qkv, seg, out_weight, bias, upstream, pre_act, down_weight,
    att_o, h0, go,
    qkv_v, seg_v, ow_v, bias_v, pre_v, slope_v, ug, uo, wg, wo, ag, ctx,
    att_p, att_r, att_h, att_f,
    hp, hh, hf, acc, gs, gr,
    ssem, rsem, lsem,
):
    y, z, x, c = (lax.axis_index(name) for name in ("y", "z", "x", "c"))
    t = 2 * x + c
    yy = [lax.rem(y + d, 4) for d in range(4)]
    zz = [lax.rem(z + d, 8) for d in range(8)]
    xx = [lax.rem(x + d, 4) for d in range(4)]
    oc = 1 - c
    sent = []

    def send(k, src, dst, **where):
        copy = pltpu.make_async_remote_copy(
            src_ref=src, dst_ref=dst, send_sem=ssem.at[k], recv_sem=rsem.at[k],
            device_id=where, device_id_type=pl.DeviceIdType.MESH,
        )
        copy.start()
        sent.append(copy)

    def arrived(k, dst, **where):
        pltpu.make_async_remote_copy(
            src_ref=dst, dst_ref=dst, send_sem=ssem.at[k], recv_sem=rsem.at[k],
            device_id=where, device_id_type=pl.DeviceIdType.MESH,
        ).wait_recv()

    def fetch(k, src, dst):
        copy = pltpu.make_async_copy(src, dst, lsem.at[k])
        copy.start()
        return copy

    got_pre = fetch(L_PRE, pre_act, pre_v)
    got_w = fetch(L_W, down_weight, wg.at[z])
    got_up = fetch(L_UP, upstream.at[:, pl.ds(pl.multiple_of(y * 1024, 1024), 1024)], ug.at[y, t])
    got_seg = fetch(L_SEG, seg, seg_v)
    got_qkv = fetch(L_QKV, qkv, qkv_v)
    got_uo = [
        fetch(L_UO + e, upstream.at[:, pl.ds(pl.multiple_of(yy[e] * 1024, 1024), 1024)], uo.at[e - 1, t])
        for e in (1, 2, 3)
    ]
    got_bias = fetch(L_BIAS, bias, bias_v)
    got_ow = fetch(L_OW, out_weight, ow_v)

    barrier = pltpu.get_barrier_semaphore()
    peers = [{"y": yy[d]} for d in (1, 2, 3)] + [{"z": zz[d]} for d in (1, 7)]
    peers += [{"x": xx[d]} for d in (1, 3)] + [{"c": oc}]
    for peer in peers:
        pl.semaphore_signal(barrier, inc=1, device_id=peer, device_id_type=pl.DeviceIdType.MESH)
    pl.semaphore_wait(barrier, len(peers))

    got_w.wait()
    send(WR, wg.at[z], wg.at[z], z=zz[1])
    send(WL, wg.at[z], wg.at[z], z=zz[7])
    for d in (1, 3, 2):
        columns = pl.ds(pl.multiple_of(yy[d] * 1024, 1024), 1024)
        send(U1 + d, upstream.at[:, columns], ug.at[y, t], y=yy[d])
    for d in (1, 3, 2):
        send(WY + d, wg.at[z, :, pl.ds(CQ, CO)], wo.at[3 - d, z], y=yy[d])
    got_up.wait()
    send(U2R, ug.at[y, t], ug.at[y, t], x=xx[1])
    send(U2L, ug.at[y, t], ug.at[y, t], x=xx[3])

    got_pre.wait()

    def gelu(q):
        def rows(i, carry):
            here = pl.ds(pl.multiple_of(q * 128 + i * 16, 16), 16)
            v = pre_v[here, :].astype(F32)
            tail = 1.0 + lax.erf(v * ROOT_HALF)
            ag[y, here, :] = (0.5 * v * tail).astype(BF)
            slope_v[here, :] = 0.5 * tail + v * jnp.exp(-0.5 * v * v) * INV_ROOT_TAU
            return carry

        lax.fori_loop(0, 8, rows, 0)

    def act_own(q):
        part = pl.ds(q * 128, 128)
        send(AR + q, ag.at[y, part], ag.at[y, part], y=yy[1])
        send(AL + q, ag.at[y, part], ag.at[y, part], y=yy[3])

    def act_hop(q):
        part = pl.ds(q * 128, 128)
        low_slot, high_slot = ag.at[yy[3], part], ag.at[yy[1], part]
        arrived(AR + q, low_slot, y=yy[3])
        if q % 2 == 0:
            send(ARF + q, low_slot, low_slot, y=yy[1])
        arrived(AL + q, high_slot, y=yy[1])
        if q % 2 == 1:
            send(ALF + q, high_slot, high_slot, y=yy[3])

    def act_far():
        for q in range(4):
            slot = ag.at[yy[2], pl.ds(q * 128, 128)]
            if q % 2 == 0:
                arrived(ARF + q, slot, y=yy[3])
            else:
                arrived(ALF + q, slot, y=yy[1])

    def own_upstream(e):
        slot = ug.at[yy[e], t]
        arrived(U1 + (4 - e), slot, y=yy[e])
        send(U2R + e, slot, slot, x=xx[1])
        send(U2L + e, slot, slot, x=xx[3])

    t_left, t_right, t_far = 2 * xx[3] + c, 2 * xx[1] + c, 2 * xx[2] + c

    def upstream_hop(e):
        left, right = ug.at[yy[e], t_left], ug.at[yy[e], t_right]
        arrived(U2R + e, left, x=xx[3])
        if e in (0, 1):
            send(U2FR + e, left, left, x=xx[1])
        arrived(U2L + e, right, x=xx[1])
        if e in (2, 3):
            send(U2FL + e, right, right, x=xx[3])

    def upstream_far():
        for e in (0, 1):
            arrived(U2FR + e, ug.at[yy[e], t_far], x=xx[3])
        for e in (3, 2):
            arrived(U2FL + e, ug.at[yy[e], t_far], x=xx[1])

    def others_own(e):
        got_uo[e - 1].wait()
        slot = uo.at[e - 1, t]
        send(UOR + e, slot, slot, x=xx[1])
        send(UOL + e, slot, slot, x=xx[3])

    first, last = pl.ds(0, 32), pl.ds(32, 32)

    def others_hop(e):
        left, right = uo.at[e - 1, t_left], uo.at[e - 1, t_right]
        arrived(UOR + e, left, x=xx[3])
        if e == 1:
            send(UOFR + e, left, left, x=xx[1])
        if e == 2:
            send(UOFR + e, left.at[first], left.at[first], x=xx[1])
        arrived(UOL + e, right, x=xx[1])
        if e == 3:
            send(UOFL + e, right, right, x=xx[3])
        if e == 2:
            send(UOFL + e, right.at[last], right.at[last], x=xx[3])

    def others_far():
        arrived(UOFR + 1, uo.at[0, t_far], x=xx[3])
        arrived(UOFR + 2, uo.at[1, t_far].at[first], x=xx[3])
        arrived(UOFL + 3, uo.at[2, t_far], x=xx[1])
        arrived(UOFL + 2, uo.at[1, t_far].at[last], x=xx[1])

    low, high = pl.ds(0, 64), pl.ds(64, 64)

    def weight_hop(s):
        from_left, from_right = zz[8 - s], zz[s]
        arrived(WR + s - 1, wg.at[from_left], z=zz[7])
        left, right = wg.at[from_left], wg.at[from_right]
        if s == 3:
            left, right = wg.at[from_left, low], wg.at[from_right, high]
        send(WR + s, left, left, z=zz[1])
        arrived(WL + s - 1, wg.at[from_right], z=zz[1])
        send(WL + s, right, right, z=zz[7])

    def weight_far():
        arrived(WR + 3, wg.at[zz[4], low], z=zz[7])
        arrived(WL + 3, wg.at[zz[4], high], z=zz[1])

    def side_own():
        for e in (1, 3, 2):
            arrived(WY + 4 - e, wo.at[e - 1, z], y=yy[e])
        send(WOR, wo.at[:, z], wo.at[:, z], z=zz[1])
        send(WOL, wo.at[:, z], wo.at[:, z], z=zz[7])

    def side_hop(s):
        from_left, from_right = zz[8 - s], zz[s]
        arrived(WOR + s - 1, wo.at[:, from_left], z=zz[7])
        left, right = wo.at[:, from_left], wo.at[:, from_right]
        if s == 3:
            left, right = wo.at[:, from_left, low], wo.at[:, from_right, high]
        send(WOR + s, left, left, z=zz[1])
        arrived(WOL + s - 1, wo.at[:, from_right], z=zz[1])
        send(WOL + s, right, right, z=zz[7])

    def side_far():
        arrived(WOR + 3, wo.at[:, zz[4], low], z=zz[7])
        arrived(WOL + 3, wo.at[:, zz[4], high], z=zz[1])

    def attend(pair):
        labels = seg_v[0].astype(F32)
        row_i = lax.broadcasted_iota(jnp.int32, (128, 1), 0)
        col_i = lax.broadcasted_iota(jnp.int32, (1, 128), 1)
        starts = [
            (64.0 - jnp.sum(labels[2 * pair + p : 2 * pair + p + 1, :], axis=1, keepdims=True)).astype(jnp.int32)
            for p in range(2)
        ]

        def image(i):
            second_pack = i >= 64
            place = jnp.where(second_pack, i - 64, i)
            bound = jnp.where(second_pack, starts[1], starts[0])
            return jnp.where(second_pack, 2, 0) + jnp.where(place >= bound, 1, 0)

        same = image(row_i) == image(col_i)
        rows = pl.ds(pair * 128, 128)
        for h in range(4):
            cols = pl.ds(h * 128, 128)
            s = lax.dot_general(
                qkv_v[0, rows, cols], qkv_v[1, rows, cols], (((1,), (1,)), ((), ())),
                preferred_element_type=F32,
            ) * SCALE
            s = jnp.where(same, s, -1e30)
            e = jnp.where(same, jnp.exp(s - jnp.max(s, axis=1, keepdims=True)), 0.0)
            w = (e / jnp.sum(e, axis=1, keepdims=True)).astype(BF)
            ctx[rows, cols] = jnp.dot(w, qkv_v[2, rows, cols], preferred_element_type=F32).astype(BF)

    def project(n, carry):
        cols = pl.ds(pl.multiple_of(n * 512, 512), 512)
        part = lax.dot_general(
            ctx[...], ow_v[cols, :], (((1,), (1,)), ((), ())), preferred_element_type=F32
        )
        att_p[:, :, :, cols] = part.astype(BF).reshape(4, 2, 64, 512)
        return carry

    def chip_sum(e):
        arrived(ATS + e, att_r.at[xx[e]], c=oc)

        def rows(i, carry):
            here = pl.ds(pl.multiple_of(i * 16, 16), 16)
            both = att_p[xx[e], c, here, :].astype(F32) + att_r[xx[e], here, :].astype(F32)
            att_p[xx[e], c, here, :] = both.astype(BF)
            return carry

        lax.fori_loop(0, 4, rows, 0)

    def att_first():
        chip_sum(2)
        for k, cols in enumerate((pl.ds(0, 2048), pl.ds(2048, 2048))):
            send(ATH + k, att_p.at[xx[2], c, :, cols], att_h.at[k], x=xx[1] if k == 0 else xx[3])
        for e in (1, 3):
            chip_sum(e)

    def att_second():
        for k, e, lo in ((0, 1, 0), (1, 3, 2048)):
            arrived(ATH + k, att_h.at[k], x=xx[3] if k == 0 else xx[1])

            def add_half(i, carry, k=k, e=e, lo=lo):
                here = pl.ds(pl.multiple_of(i * 16, 16), 16)
                cols = pl.ds(lo, 2048)
                total = att_p[xx[e], c, here, cols].astype(F32) + att_h[k, here, :].astype(F32)
                att_p[xx[e], c, here, cols] = total.astype(BF)
                return carry

            lax.fori_loop(0, 4, add_half, 0)
            send(ATF + k, att_p.at[xx[e], c], att_f.at[k], x=xx[e])

    def att_last():
        arrived(ATS, att_r.at[x], c=oc)
        for k in range(2):
            arrived(ATF + k, att_f.at[k], x=xx[3] if k == 0 else xx[1])
        got_bias.wait()
        row = bias_v[...].astype(F32).reshape(1, 4096)

        def att_rows(i, carry):
            here = pl.ds(pl.multiple_of(i * 16, 16), 16)
            total = att_p[x, c, here, :].astype(F32) + att_r[x, here, :].astype(F32)
            total = total + att_f[0, here, :].astype(F32) + att_f[1, here, :].astype(F32)
            att_o[here, :] = total + row
            return carry

        lax.fori_loop(0, 4, att_rows, 0)

    def hidden(d, store):
        def tile(n, carry):
            cols = pl.ds(pl.multiple_of(n * 256, 256), 256)
            store(
                cols,
                jnp.dot(
                    ug[yy[d]].reshape(512, 1024), wg[:, :, cols].reshape(1024, 256),
                    preferred_element_type=F32,
                ),
            )
            return carry

        lax.fori_loop(0, CQ // 256, tile, 0)

    def to_send(d):
        def store(cols, value):
            hp[d - 1, :, cols] = value.astype(BF)

        return store

    def to_keep(cols, value):
        h0[:, cols] = value

    side_cols = pl.ds(CQ, CO)

    def hidden_side():
        def rows(i, carry):
            total = jnp.dot(
                ug[y, pl.ds(2 * i, 2)].reshape(128, 1024), wg[:, :, side_cols].reshape(1024, CO),
                preferred_element_type=F32,
            )
            for e in range(3):
                total = total + jnp.dot(
                    uo[e, pl.ds(2 * i, 2)].reshape(128, 1024), wo[e].reshape(1024, CO),
                    preferred_element_type=F32,
                )
            here = pl.ds(pl.multiple_of(i * 128, 128), 128)
            h0[here, side_cols] = total * slope_v[here, side_cols]
            return carry

        lax.fori_loop(0, 4, rows, 0)

    def weight_part(e, start):
        def tile(m, carry):
            cols = pl.ds(pl.multiple_of(m * 256, 256), 256)
            part = lax.dot_general(
                ug[yy[e], :, :, cols].reshape(512, 256), ag[yy[e]], (((0,), (0,)), ((), ())),
                preferred_element_type=F32,
            ).reshape(2, 128, 1024)
            here = pl.ds(2 * m, 2)
            if start:
                acc[here] = part
            else:
                acc[here] = acc[here] + part
            return carry

        lax.fori_loop(0, 4, tile, 0)

    def weight_tile(e, i):
        m = lax.rem((z + 4) // 2 + i, 4)
        cols = pl.ds(pl.multiple_of(m * 256, 256), 256)
        part = lax.dot_general(
            ug[yy[e], :, :, cols].reshape(512, 256), ag[yy[e]], (((0,), (0,)), ((), ())),
            preferred_element_type=F32,
        ).reshape(2, 128, 1024)
        here = pl.ds(2 * m, 2)
        acc[here] = acc[here] + part

    def grad_id(k, s, half):
        return GRS + (k * 4 + s) * 2 + half

    def grad_send(k, s, half, add):
        target = zz[4 - s] if k == 0 else zz[4 + s]
        here = pl.ds(half * 64, 64)
        came = zz[7] if k == 0 else zz[1]
        if add:
            arrived(grad_id(k, s - 1, half), gr.at[k, s - 1, here], z=came)
            gs[k, s, here, :] = (acc[target, here, :] + gr[k, s - 1, here, :].astype(F32)).astype(BF)
        else:
            gs[k, s, here, :] = acc[target, here, :].astype(BF)
        send(grad_id(k, s, half), gs.at[k, s, here], gr.at[k, s, here], z=zz[1] if k == 0 else zz[7])

    top, bottom = pl.ds(0, 256), pl.ds(256, 256)

    def hidden_hop(k):
        slot, here = (0, top) if k == 0 else (2, bottom)
        arrived(HHS + k, hh.at[k], y=yy[3] if k == 0 else yy[1])
        start = 0 if k == 0 else 256

        def rows(i, carry):
            there = pl.ds(pl.multiple_of(i * 16, 16), 16)
            mine = pl.ds(pl.multiple_of(start + i * 16, 16), 16)
            total = hp[slot, mine, :].astype(F32) + hh[k, there, :].astype(F32)
            hp[slot, mine, :] = total.astype(BF)
            return carry

        lax.fori_loop(0, 16, rows, 0)
        send(HFS + 2 + k, hp.at[slot, here], hf.at[k, here], y=yy[1] if k == 0 else yy[3])

    main_cols = pl.ds(0, CQ)

    def fold(k, start):
        def rows(i, carry):
            here = pl.ds(pl.multiple_of(start + i * 16, 16), 16)
            h0[here, main_cols] = h0[here, main_cols] + hf[k, here, :].astype(F32)
            return carry

        lax.fori_loop(0, 16, rows, 0)

    def finish(k, start):
        def rows(i, carry):
            here = pl.ds(pl.multiple_of(start + i * 16, 16), 16)
            total = h0[here, main_cols] + hf[k, here, :].astype(F32)
            h0[here, main_cols] = total * slope_v[here, main_cols]
            return carry

        lax.fori_loop(0, 16, rows, 0)

    gelu(0)
    act_own(0)
    gelu(1)
    gelu(2)
    gelu(3)
    got_seg.wait()
    got_qkv.wait()
    for pair in range(4):
        attend(pair)
    weight_hop(1)
    act_own(1)
    got_ow.wait()
    lax.fori_loop(0, 3, project, 0)
    side_own()
    for e in (3, 1, 2):
        own_upstream(e)
    send(U2S, ug.at[:, t], ug.at[:, t], c=oc)
    lax.fori_loop(3, 8, project, 0)
    for e in (2, 1, 3, 0):
        send(ATS + e, att_p.at[xx[e], oc], att_r.at[xx[e]], c=oc)
    act_hop(0)
    act_own(2)
    weight_hop(2)
    upstream_hop(0)
    upstream_hop(3)
    side_hop(1)
    act_hop(1)
    act_own(3)
    upstream_hop(1)
    upstream_hop(2)
    send(U2S + 1, ug.at[:, t_left], ug.at[:, t_left], c=oc)
    send(U2S + 2, ug.at[:, t_right], ug.at[:, t_right], c=oc)
    for e in (1, 3, 2):
        others_own(e)
    send(UOS, uo.at[:, t], uo.at[:, t], c=oc)
    weight_hop(3)
    side_hop(2)
    act_hop(2)
    upstream_far()
    send(U2S + 3, ug.at[:, t_far], ug.at[:, t_far], c=oc)
    att_first()
    for k, dx in ((0, 0), (1, 3), (2, 1), (3, 2)):
        arrived(U2S + k, ug.at[:, 2 * xx[dx] + oc], c=oc)
    weight_part(0, True)
    weight_far()
    hidden(2, to_send(2))
    side_hop(3)
    act_hop(3)
    send(HHS, hp.at[1, top], hh.at[0], y=yy[1])
    send(HHS + 1, hp.at[1, bottom], hh.at[1], y=yy[3])
    for e in (1, 3, 2):
        others_hop(e)
    send(UOS + 1, uo.at[:, t_left], uo.at[:, t_left], c=oc)
    send(UOS + 2, uo.at[:, t_right], uo.at[:, t_right], c=oc)
    weight_part(3, False)
    weight_part(1, False)
    att_second()
    act_far()
    weight_tile(2, 0)
    grad_send(0, 0, 0, False)
    grad_send(1, 0, 1, False)
    lax.fori_loop(1, 4, lambda i, carry: weight_tile(2, i), None)
    grad_send(0, 1, 1, False)
    grad_send(1, 1, 0, False)
    hidden(1, to_send(1))
    send(HFS, hp.at[0, bottom], hf.at[0, bottom], y=yy[1])
    hidden(3, to_send(3))
    send(HFS + 1, hp.at[2, top], hf.at[1, top], y=yy[3])
    others_far()
    send(UOS + 3, uo.at[:, t_far], uo.at[:, t_far], c=oc)
    side_far()
    grad_send(0, 1, 0, True)
    grad_send(1, 1, 1, True)
    grad_send(0, 2, 1, True)
    grad_send(1, 2, 0, True)
    hidden_hop(0)
    hidden_hop(1)
    hidden(0, to_keep)
    grad_send(0, 2, 0, True)
    grad_send(1, 2, 1, True)
    grad_send(0, 3, 1, True)
    grad_send(1, 3, 0, True)
    for k, dx in ((0, 0), (1, 3), (2, 1), (3, 2)):
        arrived(UOS + k, uo.at[:, 2 * xx[dx] + oc], c=oc)
    hidden_side()
    grad_send(0, 3, 0, True)
    grad_send(1, 3, 1, True)
    att_last()

    arrived(HFS, hf.at[0, bottom], y=yy[3])
    arrived(HFS + 1, hf.at[1, top], y=yy[1])
    fold(0, 256)
    fold(1, 0)

    def grad_last(half):
        here = pl.ds(half * 64, 64)
        for k in range(2):
            arrived(grad_id(k, 3, half), gr.at[k, 3, here], z=zz[7] if k == 0 else zz[1])
        total = acc[z, here, :] + gr[0, 3, here, :].astype(F32) + gr[1, 3, here, :].astype(F32)
        go[here, :] = total * (1.0 / 32.0)

    grad_last(0)
    grad_last(1)
    arrived(HFS + 2, hf.at[0, top], y=yy[3])
    finish(0, 0)
    arrived(HFS + 3, hf.at[1, bottom], y=yy[1])
    finish(1, 256)

    for copy in sent:
        copy.wait_send()


def body(*args):
    hbm = pl.BlockSpec(memory_space=pltpu.HBM)
    vmem = pltpu.VMEM
    return pl.pallas_call(
        kernel,
        out_shape=(
            jax.ShapeDtypeStruct((64, 4096), F32),
            jax.ShapeDtypeStruct((512, 1024), F32),
            jax.ShapeDtypeStruct((128, 1024), F32),
        ),
        in_specs=[hbm] * 7,
        out_specs=(pl.BlockSpec(memory_space=pltpu.VMEM),) * 3,
        scratch_shapes=[
            vmem((3, 512, 512), BF),
            vmem((1, 8, 64), jnp.int32),
            vmem((4096, 512), BF),
            vmem((4096,), BF),
            vmem((512, 1024), BF),
            vmem((512, 1024), F32),
            vmem((4, 8, 64, 1024), BF),
            vmem((3, 8, 64, 1024), BF),
            vmem((8, 128, 1024), BF),
            vmem((3, 8, 128, CO), BF),
            vmem((4, 512, 1024), BF),
            vmem((512, 512), BF),
            vmem((4, 2, 64, 4096), BF),
            vmem((4, 64, 4096), BF),
            vmem((2, 64, 2048), BF),
            vmem((2, 64, 4096), BF),
            vmem((3, 512, CQ), BF),
            vmem((2, 256, CQ), BF),
            vmem((2, 512, CQ), BF),
            vmem((8, 128, 1024), F32),
            vmem((2, 4, 128, 1024), BF),
            vmem((2, 4, 128, 1024), BF),
            pltpu.SemaphoreType.DMA((N_IDS,)),
            pltpu.SemaphoreType.DMA((N_IDS,)),
            pltpu.SemaphoreType.DMA((N_LOCAL,)),
        ],
        compiler_params=pltpu.CompilerParams(
            collective_id=0, has_side_effects=True, vmem_limit_bytes=50 * 1024 * 1024
        ),
        name="layer",
    )(*(pltpu.with_memory_space_constraint(a, pltpu.HBM) for a in args))


def solution(mesh):
    finer = Mesh(mesh.devices.reshape(4, 8, 4, 2), ("y", "z", "x", "c"))
    tensor = ("x", "c")
    in_specs = (
        P(None, DP, tensor),
        P(DP, None, None),
        P(None, tensor),
        P(),
        P(DP_TENSOR, None),
        P(DP, tensor),
        P(DP, tensor),
    )
    out_specs = (P(DP_TENSOR, None), P(DP, tensor), P(DP, tensor))
    return jax.shard_map(body, mesh=finer, in_specs=in_specs, out_specs=out_specs, check_vma=False)
```

```python
import math

import jax
import jax.numpy as jnp
from jax import lax
from jax.experimental import pallas as pl
from jax.experimental.pallas import tpu as pltpu
from jax.sharding import Mesh
from jax.sharding import PartitionSpec as P

HEAD = 128
DP = ("y", "z")
DP_TENSOR = ("y", "z", "x", "c")
BF = jnp.bfloat16
F32 = jnp.float32

ROOT_HALF = 1.0 / math.sqrt(2.0)
INV_ROOT_TAU = 1.0 / math.sqrt(2.0 * math.pi)
SCALE = 1.0 / math.sqrt(HEAD)


class Ids:
    def __init__(self):
        self.n = 0

    def take(self, count=1):
        first = self.n
        self.n += count
        return first


IDS = Ids()
U1 = IDS.take(4)
UPR, UPL = IDS.take(4), IDS.take(4)
UPFR, UPFL = IDS.take(4), IDS.take(4)
UPS = IDS.take(4)
URR, URL = IDS.take(4), IDS.take(4)
URFR, URFL = IDS.take(4), IDS.take(4)
URS = IDS.take(4)
WY = IDS.take(4)
WR, WL = IDS.take(4), IDS.take(4)
WOR, WOL = IDS.take(4), IDS.take(4)
AR, AL = IDS.take(4), IDS.take(4)
ARF, ALF = IDS.take(4), IDS.take(4)
ATS = IDS.take(4)
ATH, ATF = IDS.take(2), IDS.take(2)
HHS, HFS = IDS.take(2), IDS.take(4)
GRS = IDS.take(16)
GOS = IDS.take(16)
GYS = IDS.take(4)
N_IDS = 109
N_SEND = 40

LOCAL = Ids()
L_QKV, L_SEG, L_OW, L_PRE, L_W, L_BIAS = (LOCAL.take() for _ in range(6))
L_UP = LOCAL.take(4)
N_LOCAL = LOCAL.n

CO = 256
CQ = 1024 - CO
CW = 128
CA = 1024 - CW
TOP = 288


def kernel(
    qkv, seg, out_weight, bias, upstream, pre_act, down_weight,
    att_o, h0, go,
    qkv_v, seg_v, ow_v, bias_v, pre_v, slope_v, up, ur, wg, wo, ag, ctx,
    att_p, att_r, att_h, att_f,
    hp, hh, hf, acc, gs, gr, gp, gq, gy,
    ssem, rsem, lsem,
):
    y, z, x, c = (lax.axis_index(name) for name in ("y", "z", "x", "c"))
    t = 2 * x + c
    yy = [lax.rem(y + d, 4) for d in range(4)]
    zz = [lax.rem(z + d, 8) for d in range(8)]
    xx = [lax.rem(x + d, 4) for d in range(4)]
    oc = 1 - c
    sent = []
    place = {}

    def spot(k):
        return place.setdefault(k, len(place))

    def send(k, src, dst, **where):
        n = len(sent)
        if n >= N_SEND:
            sent[n - N_SEND].wait_send()
        copy = pltpu.make_async_remote_copy(
            src_ref=src, dst_ref=dst, send_sem=ssem.at[n % N_SEND], recv_sem=rsem.at[spot(k)],
            device_id=where, device_id_type=pl.DeviceIdType.MESH,
        )
        copy.start()
        sent.append(copy)

    def arrived(k, dst, **where):
        pltpu.make_async_remote_copy(
            src_ref=dst, dst_ref=dst, send_sem=ssem.at[0], recv_sem=rsem.at[spot(k)],
            device_id=where, device_id_type=pl.DeviceIdType.MESH,
        ).wait_recv()

    def fetch(k, src, dst):
        copy = pltpu.make_async_copy(src, dst, lsem.at[k])
        copy.start()
        return copy

    got_pre = fetch(L_PRE, pre_act, pre_v)
    got_w = fetch(L_W, down_weight, wg.at[z])
    got_up = [
        fetch(L_UP + e, upstream.at[:, pl.ds(pl.multiple_of(yy[e] * 1024, 1024), 1024)], up.at[e, t])
        for e in range(4)
    ]
    got_seg = fetch(L_SEG, seg, seg_v)
    got_qkv = fetch(L_QKV, qkv, qkv_v)
    got_bias = fetch(L_BIAS, bias, bias_v)
    got_ow = fetch(L_OW, out_weight, ow_v)

    barrier = pltpu.get_barrier_semaphore()
    peers = [{"y": yy[d]} for d in (1, 2, 3)] + [{"z": zz[d]} for d in (1, 7)]
    peers += [{"x": xx[d]} for d in (1, 3)] + [{"c": oc}]
    for peer in peers:
        pl.semaphore_signal(barrier, inc=1, device_id=peer, device_id_type=pl.DeviceIdType.MESH)
    pl.semaphore_wait(barrier, len(peers))

    got_w.wait()
    send(WR, wg.at[z], wg.at[z], z=zz[1])
    send(WL, wg.at[z], wg.at[z], z=zz[7])
    for d in (1, 3, 2):
        send(WY + d, wg.at[z, :, pl.ds(CQ, CO)], wo.at[3 - d, z], y=yy[d])

    for copy in got_up:
        copy.wait()

    def own_first(e):
        send(UPR + e, up.at[e, t], up.at[e, t], x=xx[1])
        send(UPL + e, up.at[e, t], up.at[e, t], x=xx[3])

    def to_others():
        for d in (1, 3, 2):
            send(U1 + d, up.at[d, t], ur.at[3 - d, t], y=yy[d])

    own_first(0)
    own_first(1)
    got_pre.wait()

    def gelu(q):
        def rows(i, carry):
            here = pl.ds(pl.multiple_of(q * 128 + i * 16, 16), 16)
            v = pre_v[here, :].astype(F32)
            tail = 1.0 + lax.erf(v * ROOT_HALF)
            ag[y, here, :] = (0.5 * v * tail).astype(BF)
            slope_v[here, :] = 0.5 * tail + v * jnp.exp(-0.5 * v * v) * INV_ROOT_TAU
            return carry

        lax.fori_loop(0, 8, rows, 0)

    act_cols = pl.ds(0, CA)

    def act_own(q):
        mine = ag.at[y, pl.ds(q * 128, 128), act_cols]
        send(AR + q, mine, mine, y=yy[1])
        send(AL + q, mine, mine, y=yy[3])

    def act_hop(q):
        part = pl.ds(q * 128, 128)
        low_slot, high_slot = ag.at[yy[3], part, act_cols], ag.at[yy[1], part, act_cols]
        arrived(AR + q, low_slot, y=yy[3])
        if q % 2 == 0:
            send(ARF + q, low_slot, low_slot, y=yy[1])
        arrived(AL + q, high_slot, y=yy[1])
        if q % 2 == 1:
            send(ALF + q, high_slot, high_slot, y=yy[3])

    def act_far():
        for q in range(4):
            slot = ag.at[yy[2], pl.ds(q * 128, 128), act_cols]
            if q % 2 == 0:
                arrived(ARF + q, slot, y=yy[3])
            else:
                arrived(ALF + q, slot, y=yy[1])

    t_left, t_right, t_far = 2 * xx[3] + c, 2 * xx[1] + c, 2 * xx[2] + c
    first, last = pl.ds(0, 32), pl.ds(32, 32)

    def own_hop(e):
        left, right = up.at[e, t_left], up.at[e, t_right]
        arrived(UPR + e, left, x=xx[3])
        if e in (0, 1):
            send(UPFR + e, left, left, x=xx[1])
        arrived(UPL + e, right, x=xx[1])
        if e in (2, 3):
            send(UPFL + e, right, right, x=xx[3])

    def own_far():
        for e in (0, 1):
            arrived(UPFR + e, up.at[e, t_far], x=xx[3])
        for e in (2, 3):
            arrived(UPFL + e, up.at[e, t_far], x=xx[1])

    def other_first(e):
        slot = ur.at[e - 1, t]
        arrived(U1 + (4 - e), slot, y=yy[e])
        send(URR + e, slot, slot, x=xx[1])
        send(URL + e, slot, slot, x=xx[3])

    def other_hop(e):
        left, right = ur.at[e - 1, t_left], ur.at[e - 1, t_right]
        arrived(URR + e, left, x=xx[3])
        if e == 1:
            send(URFR + e, left, left, x=xx[1])
        if e == 2:
            send(URFR + e, left.at[first], left.at[first], x=xx[1])
        arrived(URL + e, right, x=xx[1])
        if e == 3:
            send(URFL + e, right, right, x=xx[3])
        if e == 2:
            send(URFL + e, right.at[last], right.at[last], x=xx[3])

    def other_far():
        arrived(URFR + 1, ur.at[0, t_far], x=xx[3])
        arrived(URFR + 2, ur.at[1, t_far].at[first], x=xx[3])
        arrived(URFL + 3, ur.at[2, t_far], x=xx[1])
        arrived(URFL + 2, ur.at[1, t_far].at[last], x=xx[1])

    def own_twin(k, slot):
        send(UPS + k, up.at[:, slot], up.at[:, slot], c=oc)

    def other_twin(k, slot):
        send(URS + k, ur.at[:, slot], ur.at[:, slot], c=oc)

    def own_all():
        for k, dx in ((0, 0), (1, 3), (2, 1), (3, 2)):
            arrived(UPS + k, up.at[:, 2 * xx[dx] + oc], c=oc)

    def other_all():
        for k, dx in ((0, 0), (1, 3), (2, 1), (3, 2)):
            arrived(URS + k, ur.at[:, 2 * xx[dx] + oc], c=oc)

    def tokens(e):
        return up.at[0] if e == 0 else ur.at[e - 1]

    low, high = pl.ds(0, 64), pl.ds(64, 64)

    def weight_hop(s):
        from_left, from_right = zz[8 - s], zz[s]
        arrived(WR + s - 1, wg.at[from_left], z=zz[7])
        left, right = wg.at[from_left], wg.at[from_right]
        if s == 3:
            left, right = wg.at[from_left, low], wg.at[from_right, high]
        send(WR + s, left, left, z=zz[1])
        arrived(WL + s - 1, wg.at[from_right], z=zz[1])
        send(WL + s, right, right, z=zz[7])

    def weight_far():
        arrived(WR + 3, wg.at[zz[4], low], z=zz[7])
        arrived(WL + 3, wg.at[zz[4], high], z=zz[1])

    def side_own():
        for e in (1, 3, 2):
            arrived(WY + 4 - e, wo.at[e - 1, z], y=yy[e])
        send(WOR, wo.at[:, z], wo.at[:, z], z=zz[1])
        send(WOL, wo.at[:, z], wo.at[:, z], z=zz[7])

    def side_hop(s):
        from_left, from_right = zz[8 - s], zz[s]
        arrived(WOR + s - 1, wo.at[:, from_left], z=zz[7])
        left, right = wo.at[:, from_left], wo.at[:, from_right]
        if s == 3:
            left, right = wo.at[:, from_left, low], wo.at[:, from_right, high]
        send(WOR + s, left, left, z=zz[1])
        arrived(WOL + s - 1, wo.at[:, from_right], z=zz[1])
        send(WOL + s, right, right, z=zz[7])

    def side_far():
        arrived(WOR + 3, wo.at[:, zz[4], low], z=zz[7])
        arrived(WOL + 3, wo.at[:, zz[4], high], z=zz[1])

    def attend(pair):
        labels = seg_v[0].astype(F32)
        row_i = lax.broadcasted_iota(jnp.int32, (128, 1), 0)
        col_i = lax.broadcasted_iota(jnp.int32, (1, 128), 1)
        starts = [
            (64.0 - jnp.sum(labels[2 * pair + p : 2 * pair + p + 1, :], axis=1, keepdims=True)).astype(jnp.int32)
            for p in range(2)
        ]

        def image(i):
            second_pack = i >= 64
            place = jnp.where(second_pack, i - 64, i)
            bound = jnp.where(second_pack, starts[1], starts[0])
            return jnp.where(second_pack, 2, 0) + jnp.where(place >= bound, 1, 0)

        same = image(row_i) == image(col_i)
        rows = pl.ds(pair * 128, 128)
        for h in range(4):
            cols = pl.ds(h * 128, 128)
            s = lax.dot_general(
                qkv_v[0, rows, cols], qkv_v[1, rows, cols], (((1,), (1,)), ((), ())),
                preferred_element_type=F32,
            ) * SCALE
            s = jnp.where(same, s, -1e30)
            e = jnp.where(same, jnp.exp(s - jnp.max(s, axis=1, keepdims=True)), 0.0)
            w = (e / jnp.sum(e, axis=1, keepdims=True)).astype(BF)
            ctx[rows, cols] = jnp.dot(w, qkv_v[2, rows, cols], preferred_element_type=F32).astype(BF)

    def project(n, carry):
        cols = pl.ds(pl.multiple_of(n * 512, 512), 512)
        part = lax.dot_general(
            ctx[...], ow_v[cols, :], (((1,), (1,)), ((), ())), preferred_element_type=F32
        )
        att_p[:, :, :, cols] = part.astype(BF).reshape(4, 2, 64, 512)
        return carry

    def chip_sum(e):
        arrived(ATS + e, att_r.at[xx[e]], c=oc)

        def rows(i, carry):
            here = pl.ds(pl.multiple_of(i * 16, 16), 16)
            both = att_p[xx[e], c, here, :].astype(F32) + att_r[xx[e], here, :].astype(F32)
            att_p[xx[e], c, here, :] = both.astype(BF)
            return carry

        lax.fori_loop(0, 4, rows, 0)

    def att_first():
        chip_sum(2)
        for k, cols in enumerate((pl.ds(0, 2048), pl.ds(2048, 2048))):
            send(ATH + k, att_p.at[xx[2], c, :, cols], att_h.at[k], x=xx[1] if k == 0 else xx[3])
        for e in (1, 3):
            chip_sum(e)

    def att_second():
        for k, e, lo in ((0, 1, 0), (1, 3, 2048)):
            arrived(ATH + k, att_h.at[k], x=xx[3] if k == 0 else xx[1])

            def add_half(i, carry, k=k, e=e, lo=lo):
                here = pl.ds(pl.multiple_of(i * 16, 16), 16)
                cols = pl.ds(lo, 2048)
                total = att_p[xx[e], c, here, cols].astype(F32) + att_h[k, here, :].astype(F32)
                att_p[xx[e], c, here, cols] = total.astype(BF)
                return carry

            lax.fori_loop(0, 4, add_half, 0)
            send(ATF + k, att_p.at[xx[e], c], att_f.at[k], x=xx[e])

    def att_last():
        arrived(ATS, att_r.at[x], c=oc)
        for k in range(2):
            arrived(ATF + k, att_f.at[k], x=xx[3] if k == 0 else xx[1])
        got_bias.wait()
        row = bias_v[...].astype(F32).reshape(1, 4096)

        def att_rows(i, carry):
            here = pl.ds(pl.multiple_of(i * 16, 16), 16)
            total = att_p[x, c, here, :].astype(F32) + att_r[x, here, :].astype(F32)
            total = total + att_f[0, here, :].astype(F32) + att_f[1, here, :].astype(F32)
            att_o[here, :] = total + row
            return carry

        lax.fori_loop(0, 4, att_rows, 0)

    def hidden(d, store):
        def tile(n, carry):
            cols = pl.ds(pl.multiple_of(n * 256, 256), 256)
            store(
                cols,
                jnp.dot(
                    tokens(d)[...].reshape(512, 1024), wg[:, :, cols].reshape(1024, 256),
                    preferred_element_type=F32,
                ),
            )
            return carry

        lax.fori_loop(0, CQ // 256, tile, 0)

    def to_send(d):
        def store(cols, value):
            hp[d - 1, :, cols] = value.astype(BF)

        return store

    def to_keep(cols, value):
        h0[:, cols] = value

    side_cols = pl.ds(CQ, CO)

    def hidden_side():
        def rows(i, carry):
            total = jnp.dot(
                up[0, pl.ds(2 * i, 2)].reshape(128, 1024), wg[:, :, side_cols].reshape(1024, CO),
                preferred_element_type=F32,
            )
            for e in range(3):
                total = total + jnp.dot(
                    up[e + 1, pl.ds(2 * i, 2)].reshape(128, 1024), wo[e].reshape(1024, CO),
                    preferred_element_type=F32,
                )
            here = pl.ds(pl.multiple_of(i * 128, 128), 128)
            h0[here, side_cols] = total * slope_v[here, side_cols]
            return carry

        lax.fori_loop(0, 4, rows, 0)

    def weight_part(e, start):
        def tile(m, carry):
            cols = pl.ds(pl.multiple_of(m * 256, 256), 256)
            part = lax.dot_general(
                tokens(e)[:, :, cols].reshape(512, 256), ag[yy[e], :, act_cols], (((0,), (0,)), ((), ())),
                preferred_element_type=F32,
            ).reshape(2, 128, CA)
            here = pl.ds(2 * m, 2)
            if start:
                acc[here] = part
            else:
                acc[here] = acc[here] + part
            return carry

        lax.fori_loop(0, 4, tile, 0)

    def weight_tile(e, i):
        m = lax.rem((z + 4) // 2 + i, 4)
        cols = pl.ds(pl.multiple_of(m * 256, 256), 256)
        part = lax.dot_general(
            tokens(e)[:, :, cols].reshape(512, 256), ag[yy[e], :, act_cols], (((0,), (0,)), ((), ())),
            preferred_element_type=F32,
        ).reshape(2, 128, CA)
        here = pl.ds(2 * m, 2)
        acc[here] = acc[here] + part

    def grad_id(k, s, half):
        return GRS + (k * 4 + s) * 2 + half

    def grad_send(k, s, half, add):
        target = zz[4 - s] if k == 0 else zz[4 + s]
        here = pl.ds(half * 64, 64)
        came = zz[7] if k == 0 else zz[1]
        if add:
            arrived(grad_id(k, s - 1, half), gr.at[k, s - 1, here], z=came)
            gs[k, s, here, :] = (acc[target, here, :] + gr[k, s - 1, here, :].astype(F32)).astype(BF)
        else:
            gs[k, s, here, :] = acc[target, here, :].astype(BF)
        send(grad_id(k, s, half), gs.at[k, s, here], gr.at[k, s, here], z=zz[1] if k == 0 else zz[7])

    def side_part(e):
        quarter = up[e].reshape(512, 1024)
        part = lax.dot_general(
            ag[y, :, pl.ds(CA, CW)], quarter, (((0,), (0,)), ((), ())), preferred_element_type=F32
        ).astype(BF)
        for k in range(8):
            gp[k, e] = part[:, k * 128 : (k + 1) * 128]

    def side_id(k, s, half):
        return GOS + (k * 4 + s) * 2 + half

    def side_send(k, s, half, add):
        target = zz[4 - s] if k == 0 else zz[4 + s]
        here = pl.ds(half * 2, 2)
        if add:
            arrived(side_id(k, s - 1, half), gq.at[k, s - 1, here], z=zz[7] if k == 0 else zz[1])
            gp[target, here] = (gp[target, here].astype(F32) + gq[k, s - 1, here].astype(F32)).astype(BF)
        send(side_id(k, s, half), gp.at[target, here], gq.at[k, s, here], z=zz[1] if k == 0 else zz[7])

    def side_sum():
        for half in (0, 1):
            here = pl.ds(half * 2, 2)
            for k in range(2):
                arrived(side_id(k, 3, half), gq.at[k, 3, here], z=zz[7] if k == 0 else zz[1])
            total = gp[z, here].astype(F32) + gq[0, 3, here].astype(F32) + gq[1, 3, here].astype(F32)
            gp[z, here] = total.astype(BF)
        for d in (2, 1, 3):
            send(GYS + d, gp.at[z, d], gy.at[d - 1], y=yy[d])

    def side_last():
        for d in (1, 2, 3):
            arrived(GYS + d, gy.at[d - 1], y=yy[4 - d])
        total = gp[z, 0].astype(F32)
        for d in range(3):
            total = total + gy[d].astype(F32)
        go[:, pl.ds(CA, CW)] = total.T * (1.0 / 32.0)

    top, bottom = pl.ds(0, TOP), pl.ds(TOP, 512 - TOP)
    hh_rows = (pl.ds(0, TOP), pl.ds(0, 512 - TOP))

    def hidden_hop(k):
        slot, here = (0, top) if k == 0 else (2, bottom)
        arrived(HHS + k, hh.at[k, hh_rows[k]], y=yy[3] if k == 0 else yy[1])
        start, count = (0, TOP // 16) if k == 0 else (TOP, (512 - TOP) // 16)

        def rows(i, carry):
            there = pl.ds(pl.multiple_of(i * 16, 16), 16)
            mine = pl.ds(pl.multiple_of(start + i * 16, 16), 16)
            total = hp[slot, mine, :].astype(F32) + hh[k, there, :].astype(F32)
            hp[slot, mine, :] = total.astype(BF)
            return carry

        lax.fori_loop(0, count, rows, 0)
        send(HFS + 2 + k, hp.at[slot, here], hf.at[k, here], y=yy[1] if k == 0 else yy[3])

    main_cols = pl.ds(0, CQ)

    def fold(k, start):
        def rows(i, carry):
            here = pl.ds(pl.multiple_of(start + i * 16, 16), 16)
            h0[here, main_cols] = h0[here, main_cols] + hf[k, here, :].astype(F32)
            return carry

        lax.fori_loop(0, (512 - TOP if start else TOP) // 16, rows, 0)

    def finish(k, start):
        def rows(i, carry):
            here = pl.ds(pl.multiple_of(start + i * 16, 16), 16)
            total = h0[here, main_cols] + hf[k, here, :].astype(F32)
            h0[here, main_cols] = total * slope_v[here, main_cols]
            return carry

        lax.fori_loop(0, (512 - TOP if start else TOP) // 16, rows, 0)

    gelu(0)
    to_others()
    gelu(1)
    gelu(2)
    gelu(3)
    act_own(0)
    got_seg.wait()
    got_qkv.wait()
    attend(0)
    attend(1)
    own_first(2)
    own_first(3)
    own_twin(0, t)
    attend(2)
    attend(3)
    weight_hop(1)
    side_own()
    own_hop(0)
    own_hop(1)
    got_ow.wait()
    lax.fori_loop(0, 3, project, 0)
    act_own(1)
    own_hop(3)
    own_hop(2)
    own_twin(1, t_left)
    own_twin(2, t_right)
    lax.fori_loop(3, 8, project, 0)
    for e in (2, 1, 3, 0):
        send(ATS + e, att_p.at[xx[e], oc], att_r.at[xx[e]], c=oc)
    act_hop(0)
    act_own(2)
    for e in (3, 1, 2):
        other_first(e)
    other_twin(0, t)
    weight_hop(2)
    side_hop(1)
    own_far()
    own_twin(3, t_far)
    act_hop(1)
    act_own(3)
    own_all()
    for e in range(4):
        side_part(e)
    side_send(0, 0, 0, False)
    side_send(1, 0, 1, False)
    side_send(0, 1, 1, False)
    side_send(1, 1, 0, False)
    weight_part(0, True)
    for e in (3, 1, 2):
        other_hop(e)
    other_twin(1, t_left)
    other_twin(2, t_right)
    weight_hop(3)
    act_hop(2)
    side_hop(2)
    side_send(0, 1, 0, True)
    side_send(1, 1, 1, True)
    side_send(0, 2, 1, True)
    side_send(1, 2, 0, True)
    other_far()
    other_twin(3, t_far)
    att_first()
    act_hop(3)
    weight_far()
    other_all()
    hidden(2, to_send(2))
    send(HHS, hp.at[1, top], hh.at[0, hh_rows[0]], y=yy[1])
    send(HHS + 1, hp.at[1, bottom], hh.at[1, hh_rows[1]], y=yy[3])
    side_send(0, 2, 0, True)
    side_send(1, 2, 1, True)
    side_send(0, 3, 1, True)
    side_send(1, 3, 0, True)
    weight_part(3, False)
    side_hop(3)
    weight_part(1, False)
    att_second()
    side_send(0, 3, 0, True)
    side_send(1, 3, 1, True)
    act_far()
    weight_tile(2, 0)
    grad_send(0, 0, 0, False)
    grad_send(1, 0, 1, False)
    lax.fori_loop(1, 4, lambda i, carry: weight_tile(2, i), None)
    grad_send(0, 1, 1, False)
    grad_send(1, 1, 0, False)
    hidden(1, to_send(1))
    send(HFS, hp.at[0, bottom], hf.at[0, bottom], y=yy[1])
    hidden(3, to_send(3))
    send(HFS + 1, hp.at[2, top], hf.at[1, top], y=yy[3])
    grad_send(0, 1, 0, True)
    grad_send(1, 1, 1, True)
    side_sum()
    grad_send(0, 2, 1, True)
    grad_send(1, 2, 0, True)
    hidden_hop(0)
    hidden_hop(1)
    hidden(0, to_keep)
    grad_send(0, 2, 0, True)
    grad_send(1, 2, 1, True)
    side_far()
    hidden_side()
    grad_send(0, 3, 1, True)
    grad_send(1, 3, 0, True)
    grad_send(0, 3, 0, True)
    grad_send(1, 3, 1, True)
    side_last()
    att_last()

    arrived(HFS, hf.at[0, bottom], y=yy[3])
    arrived(HFS + 1, hf.at[1, top], y=yy[1])
    fold(0, TOP)
    fold(1, 0)

    def grad_last(half):
        here = pl.ds(half * 64, 64)
        for k in range(2):
            arrived(grad_id(k, 3, half), gr.at[k, 3, here], z=zz[7] if k == 0 else zz[1])
        total = acc[z, here, :] + gr[0, 3, here, :].astype(F32) + gr[1, 3, here, :].astype(F32)
        go[here, act_cols] = total * (1.0 / 32.0)

    grad_last(0)
    grad_last(1)
    arrived(HFS + 2, hf.at[0, top], y=yy[3])
    finish(0, 0)
    arrived(HFS + 3, hf.at[1, bottom], y=yy[1])
    finish(1, TOP)

    for copy in sent[-N_SEND:]:
        copy.wait_send()
    assert len(place) == N_IDS, len(place)


def put(a, b, c, a_out, b_out, c_out, sem):
    copies = []
    for k, (src, dst) in enumerate(((b, b_out), (a, a_out), (c, c_out))):
        copies.append(pltpu.make_async_copy(src, dst, sem.at[k]))
        copies[-1].start()
    for copy in copies:
        copy.wait()


def body(*args):
    hbm = pl.BlockSpec(memory_space=pltpu.HBM)
    vmem = pltpu.VMEM
    in_vmem = (pl.BlockSpec(memory_space=pltpu.VMEM),) * 3
    shapes = (
        jax.ShapeDtypeStruct((64, 4096), F32),
        jax.ShapeDtypeStruct((512, 1024), F32),
        jax.ShapeDtypeStruct((128, 1024), F32),
    )
    parts = pl.pallas_call(
        kernel,
        out_shape=shapes,
        in_specs=[hbm] * 7,
        out_specs=in_vmem,
        scratch_shapes=[
            vmem((3, 512, 512), BF),
            vmem((1, 8, 64), jnp.int32),
            vmem((4096, 512), BF),
            vmem((4096,), BF),
            vmem((512, 1024), BF),
            vmem((512, 1024), F32),
            vmem((4, 8, 64, 1024), BF),
            vmem((3, 8, 64, 1024), BF),
            vmem((8, 128, 1024), BF),
            vmem((3, 8, 128, CO), BF),
            vmem((4, 512, 1024), BF),
            vmem((512, 512), BF),
            vmem((4, 2, 64, 4096), BF),
            vmem((4, 64, 4096), BF),
            vmem((2, 64, 2048), BF),
            vmem((2, 64, 4096), BF),
            vmem((3, 512, CQ), BF),
            vmem((2, TOP, CQ), BF),
            vmem((2, 512, CQ), BF),
            vmem((8, 128, CA), F32),
            vmem((2, 4, 128, CA), BF),
            vmem((2, 4, 128, CA), BF),
            vmem((8, 4, CW, 128), BF),
            vmem((2, 4, 4, CW, 128), BF),
            vmem((3, CW, 128), BF),
            pltpu.SemaphoreType.DMA((N_SEND,)),
            pltpu.SemaphoreType.DMA((N_IDS,)),
            pltpu.SemaphoreType.DMA((N_LOCAL,)),
        ],
        compiler_params=pltpu.CompilerParams(
            collective_id=0, has_side_effects=True, vmem_limit_bytes=50 * 1024 * 1024
        ),
        name="layer",
    )(*(pltpu.with_memory_space_constraint(a, pltpu.HBM) for a in args))
    return pl.pallas_call(
        put,
        out_shape=shapes,
        in_specs=in_vmem,
        out_specs=(hbm,) * 3,
        scratch_shapes=[pltpu.SemaphoreType.DMA((3,))],
        compiler_params=pltpu.CompilerParams(vmem_limit_bytes=1 * 1024 * 1024),
        name="put",
    )(*parts)


def solution(mesh):
    finer = Mesh(mesh.devices.reshape(4, 8, 4, 2), ("y", "z", "x", "c"))
    tensor = ("x", "c")
    in_specs = (
        P(None, DP, tensor),
        P(DP, None, None),
        P(None, tensor),
        P(),
        P(DP_TENSOR, None),
        P(DP, tensor),
        P(DP, tensor),
    )
    out_specs = (P(DP_TENSOR, None), P(DP, tensor), P(DP, tensor))
    return jax.shard_map(body, mesh=finer, in_specs=in_specs, out_specs=out_specs, check_vma=False)
```

```python
import math

import jax
import jax.numpy as jnp
from jax import lax
from jax.experimental import pallas as pl
from jax.experimental.pallas import tpu as pltpu
from jax.sharding import Mesh
from jax.sharding import PartitionSpec as P

HEAD = 128
DP = ("y", "z")
DP_TENSOR = ("y", "z", "x", "c")
BF = jnp.bfloat16
F32 = jnp.float32

ROOT_HALF = 1.0 / math.sqrt(2.0)
INV_ROOT_TAU = 1.0 / math.sqrt(2.0 * math.pi)
SCALE = 1.0 / math.sqrt(HEAD)


class Ids:
    def __init__(self):
        self.n = 0

    def take(self, count=1):
        first = self.n
        self.n += count
        return first


IDS = Ids()
U1 = IDS.take(4)
UPR, UPL = IDS.take(4), IDS.take(4)
UPFR, UPFL = IDS.take(4), IDS.take(4)
UPS = IDS.take(4)
URR, URL = IDS.take(4), IDS.take(4)
URFR, URFL = IDS.take(4), IDS.take(4)
URS = IDS.take(4)
WY = IDS.take(4)
WR, WL = IDS.take(4), IDS.take(4)
WOR, WOL = IDS.take(4), IDS.take(4)
AR, AL = IDS.take(4), IDS.take(4)
ARF, ALF = IDS.take(4), IDS.take(4)
ATS = IDS.take(4)
ATH, ATF = IDS.take(2), IDS.take(2)
HHS, HFS = IDS.take(2), IDS.take(4)
GRS = IDS.take(16)
GOS = IDS.take(16)
GYS = IDS.take(4)
N_IDS = 109
N_SEND = 28

LOCAL = Ids()
L_QKV, L_SEG, L_OW, L_PRE, L_W, L_BIAS = (LOCAL.take() for _ in range(6))
L_UP = LOCAL.take(4)
N_LOCAL = LOCAL.n

CO = 256
CQ = 1024 - CO
CW = 128
CA = 1024 - CW
TOP = 240


def kernel(
    qkv, seg, out_weight, bias, upstream, pre_act, down_weight,
    att_o, h0, go,
    qkv_v, seg_v, ow_v, bias_v, pre_v, slope_v, up, ur, wg, wo, ag, ctx,
    att_p, att_r, att_h, att_f,
    hp, hh, hf, acc, gs, gr, gp, gq, gy,
    ssem, rsem, lsem,
):
    y, z, x, c = (lax.axis_index(name) for name in ("y", "z", "x", "c"))
    t = 2 * x + c
    yy = [lax.rem(y + d, 4) for d in range(4)]
    zz = [lax.rem(z + d, 8) for d in range(8)]
    xx = [lax.rem(x + d, 4) for d in range(4)]
    oc = 1 - c
    sent = []
    place = {}

    def spot(k):
        return place.setdefault(k, len(place))

    def send(k, src, dst, **where):
        n = len(sent)
        if n >= N_SEND:
            sent[n - N_SEND].wait_send()
        copy = pltpu.make_async_remote_copy(
            src_ref=src, dst_ref=dst, send_sem=ssem.at[n % N_SEND], recv_sem=rsem.at[spot(k)],
            device_id=where, device_id_type=pl.DeviceIdType.MESH,
        )
        copy.start()
        sent.append(copy)

    def arrived(k, dst, **where):
        pltpu.make_async_remote_copy(
            src_ref=dst, dst_ref=dst, send_sem=ssem.at[0], recv_sem=rsem.at[spot(k)],
            device_id=where, device_id_type=pl.DeviceIdType.MESH,
        ).wait_recv()

    def fetch(k, src, dst):
        copy = pltpu.make_async_copy(src, dst, lsem.at[k])
        copy.start()
        return copy

    got_pre = fetch(L_PRE, pre_act, pre_v)
    got_w = fetch(L_W, down_weight, wg.at[z])
    got_up = [
        fetch(L_UP + e, upstream.at[:, pl.ds(pl.multiple_of(yy[e] * 1024, 1024), 1024)], up.at[e, t])
        for e in range(4)
    ]
    got_seg = fetch(L_SEG, seg, seg_v)
    got_qkv = fetch(L_QKV, qkv, qkv_v)
    got_bias = fetch(L_BIAS, bias, bias_v)
    got_ow = fetch(L_OW, out_weight, ow_v)

    barrier = pltpu.get_barrier_semaphore()
    peers = [{"y": yy[d]} for d in (1, 2, 3)] + [{"z": zz[d]} for d in (1, 7)]
    peers += [{"x": xx[d]} for d in (1, 3)] + [{"c": oc}]
    for peer in peers:
        pl.semaphore_signal(barrier, inc=1, device_id=peer, device_id_type=pl.DeviceIdType.MESH)
    pl.semaphore_wait(barrier, len(peers))

    got_w.wait()
    send(WR, wg.at[z], wg.at[z], z=zz[1])
    send(WL, wg.at[z], wg.at[z], z=zz[7])
    for d in (1, 3, 2):
        send(WY, wg.at[z, :, pl.ds(CQ, CO)], wo.at[3 - d, z], y=yy[d])

    for copy in got_up:
        copy.wait()

    def own_first(e):
        send(UPR + e, up.at[e, t], up.at[e, t], x=xx[1])
        send(UPL + e, up.at[e, t], up.at[e, t], x=xx[3])

    def to_others():
        for d in (1, 3, 2):
            send(U1 + d, up.at[d, t], ur.at[3 - d, t], y=yy[d])

    own_first(0)
    own_first(1)
    got_pre.wait()

    def gelu(q):
        def rows(i, carry):
            here = pl.ds(pl.multiple_of(q * 128 + i * 16, 16), 16)
            v = pre_v[here, :].astype(F32)
            tail = 1.0 + lax.erf(v * ROOT_HALF)
            ag[y, here, :] = (0.5 * v * tail).astype(BF)
            slope_v[here, :] = 0.5 * tail + v * jnp.exp(-0.5 * v * v) * INV_ROOT_TAU
            return carry

        lax.fori_loop(0, 8, rows, 0)

    act_cols = pl.ds(0, CA)

    def act_own(q):
        mine = ag.at[y, pl.ds(q * 128, 128), act_cols]
        send(AR + q, mine, mine, y=yy[1])
        send(AL + q, mine, mine, y=yy[3])

    def act_hop(q):
        below, above = yy[3], yy[1]
        part, half = pl.ds(q * 128, 128), pl.ds(q * 128, 64)
        arrived(AR + q, ag.at[below, part, act_cols], y=below)
        send(ARF + q, ag.at[below, half, act_cols], ag.at[below, half, act_cols], y=above)
        half = pl.ds(q * 128 + 64, 64)
        arrived(AL + q, ag.at[above, part, act_cols], y=above)
        send(ALF + q, ag.at[above, half, act_cols], ag.at[above, half, act_cols], y=below)

    def act_far():
        for q in range(4):
            arrived(ARF + q, ag.at[yy[2], pl.ds(q * 128, 64), act_cols], y=yy[3])
            arrived(ALF + q, ag.at[yy[2], pl.ds(q * 128 + 64, 64), act_cols], y=yy[1])

    t_left, t_right, t_far = 2 * xx[3] + c, 2 * xx[1] + c, 2 * xx[2] + c
    first, last = pl.ds(0, 32), pl.ds(32, 32)

    def own_hop(e):
        left, right = up.at[e, t_left], up.at[e, t_right]
        arrived(UPR + e, left, x=xx[3])
        if e in (0, 2):
            send(UPFR + e, left, left, x=xx[1])
        arrived(UPL + e, right, x=xx[1])
        if e in (1, 3):
            send(UPFL + e, right, right, x=xx[3])

    def own_far():
        for e in (0, 2):
            arrived(UPFR + e, up.at[e, t_far], x=xx[3])
        for e in (1, 3):
            arrived(UPFL + e, up.at[e, t_far], x=xx[1])

    def other_first(e):
        slot = ur.at[e - 1, t]
        arrived(U1 + (4 - e), slot, y=yy[e])
        send(URR + e, slot, slot, x=xx[1])
        send(URL + e, slot, slot, x=xx[3])

    def other_hop(e):
        left, right = ur.at[e - 1, t_left], ur.at[e - 1, t_right]
        arrived(URR + e, left, x=xx[3])
        if e == 1:
            send(URFR + e, left, left, x=xx[1])
        if e == 2:
            send(URFR + e, left.at[first], left.at[first], x=xx[1])
        arrived(URL + e, right, x=xx[1])
        if e == 3:
            send(URFL + e, right, right, x=xx[3])
        if e == 2:
            send(URFL + e, right.at[last], right.at[last], x=xx[3])

    def other_far():
        arrived(URFR + 1, ur.at[0, t_far], x=xx[3])
        arrived(URFR + 2, ur.at[1, t_far].at[first], x=xx[3])
        arrived(URFL + 3, ur.at[2, t_far], x=xx[1])
        arrived(URFL + 2, ur.at[1, t_far].at[last], x=xx[1])

    def own_twin(k, slot):
        send(UPS + k, up.at[:, slot], up.at[:, slot], c=oc)

    def other_twin(k, slot):
        send(URS + k, ur.at[:, slot], ur.at[:, slot], c=oc)

    def own_all():
        for k, dx in ((0, 0), (1, 3), (2, 1), (3, 2)):
            arrived(UPS + k, up.at[:, 2 * xx[dx] + oc], c=oc)

    def other_all():
        for k, dx in ((0, 0), (1, 3), (2, 1), (3, 2)):
            arrived(URS + k, ur.at[:, 2 * xx[dx] + oc], c=oc)

    def tokens(e):
        return up.at[0] if e == 0 else ur.at[e - 1]

    low, high = pl.ds(0, 64), pl.ds(64, 64)

    def weight_hop(s):
        from_left, from_right = zz[8 - s], zz[s]
        arrived(WR + s - 1, wg.at[from_left], z=zz[7])
        left, right = wg.at[from_left], wg.at[from_right]
        if s == 3:
            left, right = wg.at[from_left, low], wg.at[from_right, high]
        send(WR + s, left, left, z=zz[1])
        arrived(WL + s - 1, wg.at[from_right], z=zz[1])
        send(WL + s, right, right, z=zz[7])

    def weight_far():
        arrived(WR + 3, wg.at[zz[4], low], z=zz[7])
        arrived(WL + 3, wg.at[zz[4], high], z=zz[1])

    def side_own():
        arrived(WY, wo.at[:, z], y=yy[1])
        send(WOR, wo.at[:, z], wo.at[:, z], z=zz[1])
        send(WOL, wo.at[:, z], wo.at[:, z], z=zz[7])

    def side_hop(s):
        from_left, from_right = zz[8 - s], zz[s]
        arrived(WOR + s - 1, wo.at[:, from_left], z=zz[7])
        left, right = wo.at[:, from_left], wo.at[:, from_right]
        if s == 3:
            left, right = wo.at[:, from_left, low], wo.at[:, from_right, high]
        send(WOR + s, left, left, z=zz[1])
        arrived(WOL + s - 1, wo.at[:, from_right], z=zz[1])
        send(WOL + s, right, right, z=zz[7])

    def side_far():
        arrived(WOR + 3, wo.at[:, zz[4], low], z=zz[7])
        arrived(WOL + 3, wo.at[:, zz[4], high], z=zz[1])

    def attend(pair):
        labels = seg_v[0].astype(F32)
        row_i = lax.broadcasted_iota(jnp.int32, (128, 1), 0)
        col_i = lax.broadcasted_iota(jnp.int32, (1, 128), 1)
        starts = [
            (64.0 - jnp.sum(labels[2 * pair + p : 2 * pair + p + 1, :], axis=1, keepdims=True)).astype(jnp.int32)
            for p in range(2)
        ]

        def image(i):
            second_pack = i >= 64
            place = jnp.where(second_pack, i - 64, i)
            bound = jnp.where(second_pack, starts[1], starts[0])
            return jnp.where(second_pack, 2, 0) + jnp.where(place >= bound, 1, 0)

        same = image(row_i) == image(col_i)
        rows = pl.ds(pair * 128, 128)
        for h in range(4):
            cols = pl.ds(h * 128, 128)
            s = lax.dot_general(
                qkv_v[0, rows, cols], qkv_v[1, rows, cols], (((1,), (1,)), ((), ())),
                preferred_element_type=F32,
            ) * SCALE
            s = jnp.where(same, s, -1e30)
            e = jnp.where(same, jnp.exp(s - jnp.max(s, axis=1, keepdims=True)), 0.0)
            w = (e / jnp.sum(e, axis=1, keepdims=True)).astype(BF)
            ctx[rows, cols] = jnp.dot(w, qkv_v[2, rows, cols], preferred_element_type=F32).astype(BF)

    def project(n, carry):
        cols = pl.ds(pl.multiple_of(n * 512, 512), 512)
        part = lax.dot_general(
            ctx[...], ow_v[cols, :], (((1,), (1,)), ((), ())), preferred_element_type=F32
        )
        att_p[:, :, :, cols] = part.astype(BF).reshape(4, 2, 64, 512)
        return carry

    def chip_sum(e):
        arrived(ATS + e, att_r.at[xx[e]], c=oc)

        def rows(i, carry):
            here = pl.ds(pl.multiple_of(i * 16, 16), 16)
            both = att_p[xx[e], c, here, :].astype(F32) + att_r[xx[e], here, :].astype(F32)
            att_p[xx[e], c, here, :] = both.astype(BF)
            return carry

        lax.fori_loop(0, 4, rows, 0)

    def att_first():
        chip_sum(2)
        for k, cols in enumerate((pl.ds(0, 2048), pl.ds(2048, 2048))):
            send(ATH + k, att_p.at[xx[2], c, :, cols], att_h.at[k], x=xx[1] if k == 0 else xx[3])
        for e in (1, 3):
            chip_sum(e)

    def att_second():
        for k, e, lo in ((0, 1, 0), (1, 3, 2048)):
            arrived(ATH + k, att_h.at[k], x=xx[3] if k == 0 else xx[1])

            def add_half(i, carry, k=k, e=e, lo=lo):
                here = pl.ds(pl.multiple_of(i * 16, 16), 16)
                cols = pl.ds(lo, 2048)
                total = att_p[xx[e], c, here, cols].astype(F32) + att_h[k, here, :].astype(F32)
                att_p[xx[e], c, here, cols] = total.astype(BF)
                return carry

            lax.fori_loop(0, 4, add_half, 0)
            send(ATF + k, att_p.at[xx[e], c], att_f.at[k], x=xx[e])

    def att_last():
        arrived(ATS, att_r.at[x], c=oc)
        for k in range(2):
            arrived(ATF + k, att_f.at[k], x=xx[3] if k == 0 else xx[1])
        got_bias.wait()
        row = bias_v[...].astype(F32).reshape(1, 4096)

        def att_rows(i, carry):
            here = pl.ds(pl.multiple_of(i * 16, 16), 16)
            total = att_p[x, c, here, :].astype(F32) + att_r[x, here, :].astype(F32)
            total = total + att_f[0, here, :].astype(F32) + att_f[1, here, :].astype(F32)
            att_o[here, :] = total + row
            return carry

        lax.fori_loop(0, 4, att_rows, 0)

    def hidden(d, store):
        for start in range(0, CQ, 256):
            cols = pl.ds(start, 256)
            store(
                cols,
                jnp.dot(
                    tokens(d)[...].reshape(512, 1024), wg[:, :, cols].reshape(1024, 256),
                    preferred_element_type=F32,
                ),
            )

    def to_send(d):
        def store(cols, value):
            hp[d - 1, :, cols] = value.astype(BF)

        return store

    def to_keep(cols, value):
        h0[:, cols] = value

    side_cols = pl.ds(CQ, CO)

    def hidden_side():
        def rows(i, carry):
            total = jnp.dot(
                up[0, pl.ds(2 * i, 2)].reshape(128, 1024), wg[:, :, side_cols].reshape(1024, CO),
                preferred_element_type=F32,
            )
            for e in range(3):
                total = total + jnp.dot(
                    up[e + 1, pl.ds(2 * i, 2)].reshape(128, 1024), wo[e].reshape(1024, CO),
                    preferred_element_type=F32,
                )
            here = pl.ds(pl.multiple_of(i * 128, 128), 128)
            h0[here, side_cols] = total * slope_v[here, side_cols]
            return carry

        lax.fori_loop(0, 4, rows, 0)

    def weight_part(e, start):
        def tile(m, carry):
            cols = pl.ds(pl.multiple_of(m * 256, 256), 256)
            part = lax.dot_general(
                tokens(e)[:, :, cols].reshape(512, 256), ag[yy[e], :, act_cols], (((0,), (0,)), ((), ())),
                preferred_element_type=F32,
            ).reshape(2, 128, CA)
            here = pl.ds(2 * m, 2)
            if start:
                acc[here] = part
            else:
                acc[here] = acc[here] + part
            return carry

        lax.fori_loop(0, 4, tile, 0)

    def weight_tile(e, i):
        m = lax.rem((z + 4) // 2 + i, 4)
        cols = pl.ds(pl.multiple_of(m * 256, 256), 256)
        part = lax.dot_general(
            tokens(e)[:, :, cols].reshape(512, 256), ag[yy[e], :, act_cols], (((0,), (0,)), ((), ())),
            preferred_element_type=F32,
        ).reshape(2, 128, CA)
        here = pl.ds(2 * m, 2)
        acc[here] = acc[here] + part

    def grad_id(k, s, half):
        return GRS + (k * 4 + s) * 2 + half

    def grad_send(k, s, half, add):
        target = zz[4 - s] if k == 0 else zz[4 + s]
        here = pl.ds(half * 64, 64)
        came = zz[7] if k == 0 else zz[1]
        if add:
            arrived(grad_id(k, s - 1, half), gr.at[k, s - 1, here], z=came)
            gs[k, s, here, :] = (acc[target, here, :] + gr[k, s - 1, here, :].astype(F32)).astype(BF)
        else:
            gs[k, s, here, :] = acc[target, here, :].astype(BF)
        send(grad_id(k, s, half), gs.at[k, s, here], gr.at[k, s, here], z=zz[1] if k == 0 else zz[7])

    def side_part(e):
        quarter = up[e].reshape(512, 1024)
        part = lax.dot_general(
            ag[y, :, pl.ds(CA, CW)], quarter, (((0,), (0,)), ((), ())), preferred_element_type=F32
        ).astype(BF)
        for k in range(8):
            gp[k, e] = part[:, k * 128 : (k + 1) * 128]

    def side_id(k, s, half):
        return GOS + (k * 4 + s) * 2 + half

    def side_send(k, s, half, add):
        target = zz[4 - s] if k == 0 else zz[4 + s]
        here = pl.ds(half * 2, 2)
        if add:
            arrived(side_id(k, s - 1, half), gq.at[k, s - 1, here], z=zz[7] if k == 0 else zz[1])
            gp[target, here] = (gp[target, here].astype(F32) + gq[k, s - 1, here].astype(F32)).astype(BF)
        send(side_id(k, s, half), gp.at[target, here], gq.at[k, s, here], z=zz[1] if k == 0 else zz[7])

    def side_sum():
        for half in (0, 1):
            here = pl.ds(half * 2, 2)
            for k in range(2):
                arrived(side_id(k, 3, half), gq.at[k, 3, here], z=zz[7] if k == 0 else zz[1])
            total = gp[z, here].astype(F32) + gq[0, 3, here].astype(F32) + gq[1, 3, here].astype(F32)
            gp[z, here] = total.astype(BF)
        for d in (2, 1, 3):
            send(GYS, gp.at[z, d], gy.at[d - 1], y=yy[d])

    def side_last():
        arrived(GYS, gy, y=yy[1])
        total = gp[z, 0].astype(F32)
        for d in range(3):
            total = total + gy[d].astype(F32)
        go[:, pl.ds(CA, CW)] = total.T * (1.0 / 32.0)

    top, bottom = pl.ds(0, TOP), pl.ds(TOP, 512 - TOP)
    hh_rows = (pl.ds(0, TOP), pl.ds(0, 512 - TOP))

    def hidden_hop(k):
        slot, here = (0, top) if k == 0 else (2, bottom)
        arrived(HHS + k, hh.at[k, hh_rows[k]], y=yy[3] if k == 0 else yy[1])
        start, count = (0, TOP // 16) if k == 0 else (TOP, (512 - TOP) // 16)

        def rows(i, carry):
            there = pl.ds(pl.multiple_of(i * 16, 16), 16)
            mine = pl.ds(pl.multiple_of(start + i * 16, 16), 16)
            total = hp[slot, mine, :].astype(F32) + hh[k, there, :].astype(F32)
            hp[slot, mine, :] = total.astype(BF)
            return carry

        lax.fori_loop(0, count, rows, 0)
        send(HFS + 2 + k, hp.at[slot, here], hf.at[k, here], y=yy[1] if k == 0 else yy[3])

    main_cols = pl.ds(0, CQ)

    def fold(k, start):
        def rows(i, carry):
            here = pl.ds(pl.multiple_of(start + i * 16, 16), 16)
            h0[here, main_cols] = h0[here, main_cols] + hf[k, here, :].astype(F32)
            return carry

        lax.fori_loop(0, (512 - TOP if start else TOP) // 16, rows, 0)

    def finish(k, start):
        def rows(i, carry):
            here = pl.ds(pl.multiple_of(start + i * 16, 16), 16)
            total = h0[here, main_cols] + hf[k, here, :].astype(F32)
            h0[here, main_cols] = total * slope_v[here, main_cols]
            return carry

        lax.fori_loop(0, (512 - TOP if start else TOP) // 16, rows, 0)

    own_first(2)
    gelu(0)
    gelu(3)
    to_others()
    act_own(0)
    side_own()
    gelu(2)
    own_first(3)
    gelu(1)
    weight_hop(1)
    own_twin(0, t)
    own_hop(1)
    own_hop(2)
    own_hop(0)
    got_seg.wait()
    got_qkv.wait()
    attend(3)
    side_hop(1)
    act_own(1)
    own_hop(3)
    attend(1)
    attend(0)
    act_own(2)
    other_first(3)
    attend(2)
    own_twin(1, t_left)
    weight_hop(2)
    other_first(2)
    got_ow.wait()
    lax.fori_loop(0, 1, project, 0)
    act_own(3)
    own_far()
    other_first(1)
    own_twin(2, t_right)
    lax.fori_loop(1, 2, project, 0)
    own_twin(3, t_far)
    lax.fori_loop(2, 6, project, 0)
    own_all()
    lax.fori_loop(6, 7, project, 0)
    for e in range(4):
        side_part(e)
    side_send(0, 0, 0, False)
    side_send(1, 0, 1, False)
    side_send(0, 1, 1, False)
    side_send(1, 1, 0, False)
    other_hop(3)
    other_twin(0, t)
    lax.fori_loop(7, 8, project, 0)
    weight_part(0, True)
    other_hop(2)
    act_hop(0)
    other_hop(1)
    act_hop(1)
    for e in (2, 1, 3, 0):
        send(ATS + e, att_p.at[xx[e], oc], att_r.at[xx[e]], c=oc)
    weight_hop(3)
    other_twin(1, t_left)
    act_hop(2)
    side_send(0, 1, 0, True)
    side_send(1, 1, 1, True)
    act_hop(3)
    att_first()
    other_twin(2, t_right)
    side_hop(2)
    side_send(0, 2, 1, True)
    side_send(1, 2, 0, True)
    other_far()
    other_twin(3, t_far)
    weight_far()
    other_all()
    hidden(2, to_send(2))
    send(HHS, hp.at[1, top], hh.at[0, hh_rows[0]], y=yy[1])
    send(HHS + 1, hp.at[1, bottom], hh.at[1, hh_rows[1]], y=yy[3])
    side_send(0, 2, 0, True)
    side_send(1, 2, 1, True)
    weight_part(3, False)
    weight_part(1, False)
    act_far()
    side_hop(3)
    weight_tile(2, 0)
    grad_send(0, 0, 0, False)
    grad_send(1, 0, 1, False)
    hidden(3, to_send(3))
    send(HFS + 1, hp.at[2, top], hf.at[1, top], y=yy[3])
    side_send(0, 3, 1, True)
    side_send(1, 3, 0, True)
    hidden(1, to_send(1))
    send(HFS, hp.at[0, bottom], hf.at[0, bottom], y=yy[1])
    lax.fori_loop(1, 4, lambda i, carry: weight_tile(2, i), None)
    side_far()
    att_second()
    side_send(0, 3, 0, True)
    side_send(1, 3, 1, True)
    grad_send(0, 1, 1, False)
    grad_send(1, 1, 0, False)
    grad_send(0, 1, 0, True)
    grad_send(1, 1, 1, True)
    side_sum()
    hidden_hop(0)
    hidden_hop(1)
    hidden(0, to_keep)
    grad_send(0, 2, 1, True)
    grad_send(1, 2, 0, True)
    grad_send(0, 2, 0, True)
    grad_send(1, 2, 1, True)
    arrived(HFS, hf.at[0, bottom], y=yy[3])
    fold(0, TOP)
    arrived(HFS + 1, hf.at[1, top], y=yy[1])
    fold(1, 0)
    side_last()
    grad_send(0, 3, 1, True)
    grad_send(1, 3, 0, True)
    hidden_side()
    grad_send(0, 3, 0, True)
    grad_send(1, 3, 1, True)
    att_last()

    def grad_last(half):
        here = pl.ds(half * 64, 64)
        for k in range(2):
            arrived(grad_id(k, 3, half), gr.at[k, 3, here], z=zz[7] if k == 0 else zz[1])
        total = acc[z, here, :] + gr[0, 3, here, :].astype(F32) + gr[1, 3, here, :].astype(F32)
        go[here, act_cols] = total * (1.0 / 32.0)

    grad_last(0)
    grad_last(1)
    arrived(HFS + 2, hf.at[0, top], y=yy[3])
    finish(0, 0)
    arrived(HFS + 3, hf.at[1, bottom], y=yy[1])
    finish(1, TOP)

    for copy in sent[-N_SEND:]:
        copy.wait_send()
    assert len(place) == N_IDS, len(place)


def put(a, b, c, a_out, b_out, c_out, sem):
    copies = []
    pieces = [(b, b_out, i * 128, 128) for i in range(4)] + [(a, a_out, i * 16, 16) for i in range(4)]
    for k, (src, dst, start, rows) in enumerate(pieces + [(c, c_out, 0, 128)]):
        here = pl.ds(start, rows)
        copies.append(pltpu.make_async_copy(src.at[here], dst.at[here], sem.at[k]))
        copies[-1].start()
    for copy in copies:
        copy.wait()


def body(*args):
    hbm = pl.BlockSpec(memory_space=pltpu.HBM)
    vmem = pltpu.VMEM
    in_vmem = (pl.BlockSpec(memory_space=pltpu.VMEM),) * 3
    shapes = (
        jax.ShapeDtypeStruct((64, 4096), F32),
        jax.ShapeDtypeStruct((512, 1024), F32),
        jax.ShapeDtypeStruct((128, 1024), F32),
    )
    parts = pl.pallas_call(
        kernel,
        out_shape=shapes,
        in_specs=[hbm] * 7,
        out_specs=in_vmem,
        scratch_shapes=[
            vmem((3, 512, 512), BF),
            vmem((1, 8, 64), jnp.int32),
            vmem((4096, 512), BF),
            vmem((4096,), BF),
            vmem((512, 1024), BF),
            vmem((512, 1024), F32),
            vmem((4, 8, 64, 1024), BF),
            vmem((3, 8, 64, 1024), BF),
            vmem((8, 128, 1024), BF),
            vmem((3, 8, 128, CO), BF),
            vmem((4, 512, 1024), BF),
            vmem((512, 512), BF),
            vmem((4, 2, 64, 4096), BF),
            vmem((4, 64, 4096), BF),
            vmem((2, 64, 2048), BF),
            vmem((2, 64, 4096), BF),
            vmem((3, 512, CQ), BF),
            vmem((2, max(TOP, 512 - TOP), CQ), BF),
            vmem((2, 512, CQ), BF),
            vmem((8, 128, CA), F32),
            vmem((2, 4, 128, CA), BF),
            vmem((2, 4, 128, CA), BF),
            vmem((8, 4, CW, 128), BF),
            vmem((2, 4, 4, CW, 128), BF),
            vmem((3, CW, 128), BF),
            pltpu.SemaphoreType.DMA((N_SEND,)),
            pltpu.SemaphoreType.DMA((N_IDS,)),
            pltpu.SemaphoreType.DMA((N_LOCAL,)),
        ],
        compiler_params=pltpu.CompilerParams(
            collective_id=0, has_side_effects=True, vmem_limit_bytes=50 * 1024 * 1024
        ),
        name="layer",
    )(*(pltpu.with_memory_space_constraint(a, pltpu.HBM) for a in args))
    return pl.pallas_call(
        put,
        out_shape=shapes,
        in_specs=in_vmem,
        out_specs=(hbm,) * 3,
        scratch_shapes=[pltpu.SemaphoreType.DMA((9,))],
        compiler_params=pltpu.CompilerParams(vmem_limit_bytes=1 * 1024 * 1024),
        name="put",
    )(*parts)


def solution(mesh):
    finer = Mesh(mesh.devices.reshape(4, 8, 4, 2), ("y", "z", "x", "c"))
    tensor = ("x", "c")
    in_specs = (
        P(None, DP, tensor),
        P(DP, None, None),
        P(None, tensor),
        P(),
        P(DP_TENSOR, None),
        P(DP, tensor),
        P(DP, tensor),
    )
    out_specs = (P(DP_TENSOR, None), P(DP, tensor), P(DP, tensor))
    return jax.shard_map(body, mesh=finer, in_specs=in_specs, out_specs=out_specs, check_vma=False)
```

```python
import math

import jax
import jax.numpy as jnp
from jax import lax
from jax.experimental import pallas as pl
from jax.experimental.pallas import tpu as pltpu
from jax.sharding import Mesh
from jax.sharding import PartitionSpec as P

HEAD = 128
DP = ("y", "z")
DP_TENSOR = ("y", "z", "x", "c")
BF = jnp.bfloat16
F32 = jnp.float32

ROOT_HALF = 1.0 / math.sqrt(2.0)
INV_ROOT_TAU = 1.0 / math.sqrt(2.0 * math.pi)
SCALE = 1.0 / math.sqrt(HEAD)


class Ids:
    def __init__(self):
        self.n = 0

    def take(self, count=1):
        first = self.n
        self.n += count
        return first


IDS = Ids()
U1 = IDS.take(4)
UPR, UPL = IDS.take(4), IDS.take(4)
UPFR, UPFL = IDS.take(4), IDS.take(4)
UPS = IDS.take(4)
URR, URL = IDS.take(4), IDS.take(4)
URFR, URFL = IDS.take(4), IDS.take(4)
URS = IDS.take(4)
WY = IDS.take(4)
WR, WL = IDS.take(4), IDS.take(4)
WOR, WOL = IDS.take(4), IDS.take(4)
AR, AL = IDS.take(4), IDS.take(4)
ARF, ALF = IDS.take(4), IDS.take(4)
ATS = IDS.take(4)
ATH, ATF = IDS.take(2), IDS.take(2)
HHS, HFS = IDS.take(2), IDS.take(4)
GRS = IDS.take(16)
GOS = IDS.take(16)
GYS = IDS.take(4)
N_IDS = 105
N_SEND = 22

LOCAL = Ids()
L_QKV, L_SEG, L_OW, L_PRE, L_W, L_BIAS = (LOCAL.take() for _ in range(6))
L_UP = LOCAL.take()
N_LOCAL = LOCAL.n

CO = 256
CQ = 1024 - CO
CW = 128
CA = 1024 - CW
TOP = 240


def kernel(
    qkv, seg, out_weight, bias, upstream, pre_act, down_weight,
    att_o, h0, go,
    qkv_v, seg_v, ow_v, bias_v, pre_v, slope_v, up, ur, wg, wo, ag, ctx,
    att_p, att_r, att_h, att_f,
    hp, hh, hf, acc, gs, gr, gp, gq, gy,
    ssem, rsem, lsem,
):
    y, z, x, c = (lax.axis_index(name) for name in ("y", "z", "x", "c"))
    t = 2 * x + c
    yy = [lax.rem(y + d, 4) for d in range(4)]
    zz = [lax.rem(z + d, 8) for d in range(8)]
    xx = [lax.rem(x + d, 4) for d in range(4)]
    oc = 1 - c
    sent = []
    place = {}

    def spot(k):
        return place.setdefault(k, len(place))

    def send(k, src, dst, **where):
        n = len(sent)
        if n >= N_SEND:
            sent[n - N_SEND].wait_send()
        copy = pltpu.make_async_remote_copy(
            src_ref=src, dst_ref=dst, send_sem=ssem.at[n % N_SEND], recv_sem=rsem.at[spot(k)],
            device_id=where, device_id_type=pl.DeviceIdType.MESH,
        )
        copy.start()
        sent.append(copy)

    def arrived(k, dst, **where):
        pltpu.make_async_remote_copy(
            src_ref=dst, dst_ref=dst, send_sem=ssem.at[0], recv_sem=rsem.at[spot(k)],
            device_id=where, device_id_type=pl.DeviceIdType.MESH,
        ).wait_recv()

    def fetch(k, src, dst):
        copy = pltpu.make_async_copy(src, dst, lsem.at[k])
        copy.start()
        return copy

    barrier = pltpu.get_barrier_semaphore()
    peers = [{"y": yy[d]} for d in (1, 2, 3)] + [{"z": zz[d]} for d in (1, 7)]
    peers += [{"x": xx[d]} for d in (1, 3)] + [{"c": oc}]
    for peer in peers:
        pl.semaphore_signal(barrier, inc=1, device_id=peer, device_id_type=pl.DeviceIdType.MESH)

    got_pre = fetch(L_PRE, pre_act, pre_v)
    got_w = fetch(L_W, down_weight, wg.at[z])
    got_up = [
        fetch(L_UP, upstream.at[:, pl.ds(pl.multiple_of(yy[e] * 1024, 1024), 1024)], up.at[e, t])
        for e in range(4)
    ]
    got_seg = fetch(L_SEG, seg, seg_v)
    got_qkv = fetch(L_QKV, qkv, qkv_v)
    got_bias = fetch(L_BIAS, bias, bias_v)
    got_ow = fetch(L_OW, out_weight, ow_v)

    pl.semaphore_wait(barrier, len(peers))

    got_w.wait()
    send(WR, wg.at[z], wg.at[z], z=zz[1])
    send(WL, wg.at[z], wg.at[z], z=zz[7])
    for d in (1, 3, 2):
        send(WY, wg.at[z, :, pl.ds(CQ, CO)], wo.at[3 - d, z], y=yy[d])

    pltpu.make_async_copy(up.at[:, t], up.at[:, t], lsem.at[L_UP]).wait()

    def own_first(e):
        send(UPR + e, up.at[e, t], up.at[e, t], x=xx[1])
        send(UPL + e, up.at[e, t], up.at[e, t], x=xx[3])

    def to_others():
        for d in (1, 3, 2):
            send(U1 + d, up.at[d, t], ur.at[3 - d, t], y=yy[d])

    own_first(0)
    own_first(1)
    got_pre.wait()

    def gelu(q):
        def rows(i, carry):
            here = pl.ds(pl.multiple_of(q * 128 + i * 16, 16), 16)
            v = pre_v[here, :].astype(F32)
            tail = 1.0 + lax.erf(v * ROOT_HALF)
            ag[y, here, :] = (0.5 * v * tail).astype(BF)
            slope_v[here, :] = 0.5 * tail + v * jnp.exp(-0.5 * v * v) * INV_ROOT_TAU
            return carry

        lax.fori_loop(0, 8, rows, 0)

    act_cols = pl.ds(0, CA)

    def act_own(q):
        mine = ag.at[y, pl.ds(q * 128, 128), act_cols]
        send(AR + q, mine, mine, y=yy[1])
        send(AL + q, mine, mine, y=yy[3])

    def act_hop(q):
        below, above = yy[3], yy[1]
        part = pl.ds(q * 128, 128)
        low_slot, high_slot = ag.at[below, part, act_cols], ag.at[above, part, act_cols]
        arrived(AR + q, low_slot, y=below)
        if q % 2 == 0:
            send(ARF + q, low_slot, low_slot, y=above)
        arrived(AL + q, high_slot, y=above)
        if q % 2 == 1:
            send(ALF + q, high_slot, high_slot, y=below)

    def act_far():
        for q in range(4):
            slot = ag.at[yy[2], pl.ds(q * 128, 128), act_cols]
            if q % 2 == 0:
                arrived(ARF + q, slot, y=yy[3])
            else:
                arrived(ALF + q, slot, y=yy[1])

    t_left, t_right, t_far = 2 * xx[3] + c, 2 * xx[1] + c, 2 * xx[2] + c
    first, last = pl.ds(0, 32), pl.ds(32, 32)

    def own_hop(e):
        left, right = up.at[e, t_left], up.at[e, t_right]
        arrived(UPR + e, left, x=xx[3])
        if e in (0, 2):
            send(UPFR + e, left, left, x=xx[1])
        arrived(UPL + e, right, x=xx[1])
        if e in (1, 3):
            send(UPFL + e, right, right, x=xx[3])

    def own_far():
        for e in (0, 2):
            arrived(UPFR + e, up.at[e, t_far], x=xx[3])
        for e in (1, 3):
            arrived(UPFL + e, up.at[e, t_far], x=xx[1])

    def other_first(e):
        slot = ur.at[e - 1, t]
        arrived(U1 + (4 - e), slot, y=yy[e])
        send(URR + e, slot, slot, x=xx[1])
        send(URL + e, slot, slot, x=xx[3])

    def other_hop(e):
        left, right = ur.at[e - 1, t_left], ur.at[e - 1, t_right]
        arrived(URR + e, left, x=xx[3])
        if e == 1:
            send(URFR + e, left, left, x=xx[1])
        if e == 2:
            send(URFR + e, left.at[first], left.at[first], x=xx[1])
        arrived(URL + e, right, x=xx[1])
        if e == 3:
            send(URFL + e, right, right, x=xx[3])
        if e == 2:
            send(URFL + e, right.at[last], right.at[last], x=xx[3])

    def other_far():
        arrived(URFR + 1, ur.at[0, t_far], x=xx[3])
        arrived(URFR + 2, ur.at[1, t_far].at[first], x=xx[3])
        arrived(URFL + 3, ur.at[2, t_far], x=xx[1])
        arrived(URFL + 2, ur.at[1, t_far].at[last], x=xx[1])

    def own_twin(k, slot):
        send(UPS + k, up.at[:, slot], up.at[:, slot], c=oc)

    def other_twin(k, slot):
        send(URS + k, ur.at[:, slot], ur.at[:, slot], c=oc)

    def own_all():
        for k, dx in ((0, 0), (1, 3), (2, 1), (3, 2)):
            arrived(UPS + k, up.at[:, 2 * xx[dx] + oc], c=oc)

    def other_all():
        for k, dx in ((0, 0), (1, 3), (2, 1), (3, 2)):
            arrived(URS + k, ur.at[:, 2 * xx[dx] + oc], c=oc)

    def tokens(e):
        return up.at[0] if e == 0 else ur.at[e - 1]

    low, high = pl.ds(0, 64), pl.ds(64, 64)

    def weight_hop(s):
        from_left, from_right = zz[8 - s], zz[s]
        arrived(WR + s - 1, wg.at[from_left], z=zz[7])
        left, right = wg.at[from_left], wg.at[from_right]
        if s == 3:
            left, right = wg.at[from_left, low], wg.at[from_right, high]
        send(WR + s, left, left, z=zz[1])
        arrived(WL + s - 1, wg.at[from_right], z=zz[1])
        send(WL + s, right, right, z=zz[7])

    def weight_far():
        arrived(WR + 3, wg.at[zz[4], low], z=zz[7])
        arrived(WL + 3, wg.at[zz[4], high], z=zz[1])

    def side_own():
        arrived(WY, wo.at[:, z], y=yy[1])
        send(WOR, wo.at[:, z], wo.at[:, z], z=zz[1])
        send(WOL, wo.at[:, z], wo.at[:, z], z=zz[7])

    def side_hop(s):
        from_left, from_right = zz[8 - s], zz[s]
        arrived(WOR + s - 1, wo.at[:, from_left], z=zz[7])
        left, right = wo.at[:, from_left], wo.at[:, from_right]
        if s == 3:
            left, right = wo.at[:, from_left, low], wo.at[:, from_right, high]
        send(WOR + s, left, left, z=zz[1])
        arrived(WOL + s - 1, wo.at[:, from_right], z=zz[1])
        send(WOL + s, right, right, z=zz[7])

    def side_far():
        arrived(WOR + 3, wo.at[:, zz[4], low], z=zz[7])
        arrived(WOL + 3, wo.at[:, zz[4], high], z=zz[1])

    def attend(pair):
        labels = seg_v[0].astype(F32)
        row_i = lax.broadcasted_iota(jnp.int32, (128, 1), 0)
        col_i = lax.broadcasted_iota(jnp.int32, (1, 128), 1)
        starts = [
            (64.0 - jnp.sum(labels[2 * pair + p : 2 * pair + p + 1, :], axis=1, keepdims=True)).astype(jnp.int32)
            for p in range(2)
        ]

        def image(i):
            second_pack = i >= 64
            place = jnp.where(second_pack, i - 64, i)
            bound = jnp.where(second_pack, starts[1], starts[0])
            return jnp.where(second_pack, 2, 0) + jnp.where(place >= bound, 1, 0)

        same = image(row_i) == image(col_i)
        rows = pl.ds(pair * 128, 128)
        for h in range(4):
            cols = pl.ds(h * 128, 128)
            s = lax.dot_general(
                qkv_v[0, rows, cols], qkv_v[1, rows, cols], (((1,), (1,)), ((), ())),
                preferred_element_type=F32,
            ) * SCALE
            s = jnp.where(same, s, -1e30)
            e = jnp.where(same, jnp.exp(s - jnp.max(s, axis=1, keepdims=True)), 0.0)
            w = (e / jnp.sum(e, axis=1, keepdims=True)).astype(BF)
            ctx[rows, cols] = jnp.dot(w, qkv_v[2, rows, cols], preferred_element_type=F32).astype(BF)

    def project(n, carry):
        cols = pl.ds(pl.multiple_of(n * 512, 512), 512)
        part = lax.dot_general(
            ctx[...], ow_v[cols, :], (((1,), (1,)), ((), ())), preferred_element_type=F32
        )
        att_p[:, :, :, cols] = part.astype(BF).reshape(4, 2, 64, 512)
        return carry

    def chip_sum(e):
        arrived(ATS + e, att_r.at[xx[e]], c=oc)

        def rows(i, carry):
            here = pl.ds(pl.multiple_of(i * 16, 16), 16)
            both = att_p[xx[e], c, here, :].astype(F32) + att_r[xx[e], here, :].astype(F32)
            att_p[xx[e], c, here, :] = both.astype(BF)
            return carry

        lax.fori_loop(0, 4, rows, 0)

    def att_first():
        chip_sum(2)
        for k, cols in enumerate((pl.ds(0, 2048), pl.ds(2048, 2048))):
            send(ATH + k, att_p.at[xx[2], c, :, cols], att_h.at[k], x=xx[1] if k == 0 else xx[3])
        for e in (1, 3):
            chip_sum(e)

    def att_second():
        for k, e, lo in ((0, 1, 0), (1, 3, 2048)):
            arrived(ATH + k, att_h.at[k], x=xx[3] if k == 0 else xx[1])

            def add_half(i, carry, k=k, e=e, lo=lo):
                here = pl.ds(pl.multiple_of(i * 16, 16), 16)
                cols = pl.ds(lo, 2048)
                total = att_p[xx[e], c, here, cols].astype(F32) + att_h[k, here, :].astype(F32)
                att_p[xx[e], c, here, cols] = total.astype(BF)
                return carry

            lax.fori_loop(0, 4, add_half, 0)
            send(ATF + k, att_p.at[xx[e], c], att_f.at[k], x=xx[e])

    def att_last():
        arrived(ATS, att_r.at[x], c=oc)
        for k in range(2):
            arrived(ATF + k, att_f.at[k], x=xx[3] if k == 0 else xx[1])
        got_bias.wait()
        row = bias_v[...].astype(F32).reshape(1, 4096)

        def att_rows(i, carry):
            here = pl.ds(pl.multiple_of(i * 16, 16), 16)
            total = att_p[x, c, here, :].astype(F32) + att_r[x, here, :].astype(F32)
            total = total + att_f[0, here, :].astype(F32) + att_f[1, here, :].astype(F32)
            att_o[here, :] = total + row
            return carry

        lax.fori_loop(0, 4, att_rows, 0)

    def hidden(d, store):
        for start in range(0, CQ, 256):
            cols = pl.ds(start, 256)
            store(
                cols,
                jnp.dot(
                    tokens(d)[...].reshape(512, 1024), wg[:, :, cols].reshape(1024, 256),
                    preferred_element_type=F32,
                ),
            )

    def to_send(d):
        def store(cols, value):
            hp[d - 1, :, cols] = value.astype(BF)

        return store

    def to_keep(cols, value):
        h0[:, cols] = value

    side_cols = pl.ds(CQ, CO)

    def hidden_side():
        def rows(i, carry):
            total = jnp.dot(
                up[0, pl.ds(2 * i, 2)].reshape(128, 1024), wg[:, :, side_cols].reshape(1024, CO),
                preferred_element_type=F32,
            )
            for e in range(3):
                total = total + jnp.dot(
                    up[e + 1, pl.ds(2 * i, 2)].reshape(128, 1024), wo[e].reshape(1024, CO),
                    preferred_element_type=F32,
                )
            here = pl.ds(pl.multiple_of(i * 128, 128), 128)
            h0[here, side_cols] = total * slope_v[here, side_cols]
            return carry

        lax.fori_loop(0, 4, rows, 0)

    def weight_part(e, start):
        def tile(m, carry):
            cols = pl.ds(pl.multiple_of(m * 256, 256), 256)
            part = lax.dot_general(
                tokens(e)[:, :, cols].reshape(512, 256), ag[yy[e], :, act_cols], (((0,), (0,)), ((), ())),
                preferred_element_type=F32,
            ).reshape(2, 128, CA)
            here = pl.ds(2 * m, 2)
            if start:
                acc[here] = part
            else:
                acc[here] = acc[here] + part
            return carry

        lax.fori_loop(0, 4, tile, 0)

    def weight_tile(e, i):
        m = lax.rem((z + 4) // 2 + i, 4)
        cols = pl.ds(pl.multiple_of(m * 256, 256), 256)
        part = lax.dot_general(
            tokens(e)[:, :, cols].reshape(512, 256), ag[yy[e], :, act_cols], (((0,), (0,)), ((), ())),
            preferred_element_type=F32,
        ).reshape(2, 128, CA)
        here = pl.ds(2 * m, 2)
        acc[here] = acc[here] + part

    def grad_id(k, s, half):
        return GRS + (k * 4 + s) * 2 + half

    def grad_send(k, s, half, add):
        target = zz[4 - s] if k == 0 else zz[4 + s]
        here = pl.ds(half * 64, 64)
        came = zz[7] if k == 0 else zz[1]
        if add:
            arrived(grad_id(k, s - 1, half), gr.at[k, s - 1, here], z=came)
            gs[k, s, here, :] = (acc[target, here, :] + gr[k, s - 1, here, :].astype(F32)).astype(BF)
        else:
            gs[k, s, here, :] = acc[target, here, :].astype(BF)
        send(grad_id(k, s, half), gs.at[k, s, here], gr.at[k, s, here], z=zz[1] if k == 0 else zz[7])

    def side_part(e):
        quarter = up[e].reshape(512, 1024)
        part = lax.dot_general(
            ag[y, :, pl.ds(CA, CW)], quarter, (((0,), (0,)), ((), ())), preferred_element_type=F32
        ).astype(BF)
        for k in range(8):
            gp[k, e] = part[:, k * 128 : (k + 1) * 128]

    def side_id(k, s, half):
        return GOS + (k * 4 + s) * 2 + half

    def side_send(k, s, half, add):
        target = zz[4 - s] if k == 0 else zz[4 + s]
        here = pl.ds(half * 2, 2)
        if add:
            arrived(side_id(k, s - 1, half), gq.at[k, s - 1, here], z=zz[7] if k == 0 else zz[1])
            gp[target, here] = (gp[target, here].astype(F32) + gq[k, s - 1, here].astype(F32)).astype(BF)
        send(side_id(k, s, half), gp.at[target, here], gq.at[k, s, here], z=zz[1] if k == 0 else zz[7])

    def side_sum():
        for half in (0, 1):
            here = pl.ds(half * 2, 2)
            for k in range(2):
                arrived(side_id(k, 3, half), gq.at[k, 3, here], z=zz[7] if k == 0 else zz[1])
            total = gp[z, here].astype(F32) + gq[0, 3, here].astype(F32) + gq[1, 3, here].astype(F32)
            gp[z, here] = total.astype(BF)
        for d in (2, 1, 3):
            send(GYS, gp.at[z, d], gy.at[d - 1], y=yy[d])

    def side_last():
        arrived(GYS, gy, y=yy[1])
        total = gp[z, 0].astype(F32)
        for d in range(3):
            total = total + gy[d].astype(F32)
        go[:, pl.ds(CA, CW)] = total.T * (1.0 / 32.0)

    top, bottom = pl.ds(0, TOP), pl.ds(TOP, 512 - TOP)
    hh_rows = (pl.ds(0, TOP), pl.ds(0, 512 - TOP))

    def hidden_hop(k):
        slot, here = (0, top) if k == 0 else (2, bottom)
        arrived(HHS + k, hh.at[k, hh_rows[k]], y=yy[3] if k == 0 else yy[1])
        start, count = (0, TOP // 16) if k == 0 else (TOP, (512 - TOP) // 16)

        def rows(i, carry):
            there = pl.ds(pl.multiple_of(i * 16, 16), 16)
            mine = pl.ds(pl.multiple_of(start + i * 16, 16), 16)
            total = hp[slot, mine, :].astype(F32) + hh[k, there, :].astype(F32)
            hp[slot, mine, :] = total.astype(BF)
            return carry

        lax.fori_loop(0, count, rows, 0)
        send(HFS + 2 + k, hp.at[slot, here], hf.at[k, here], y=yy[1] if k == 0 else yy[3])

    main_cols = pl.ds(0, CQ)

    def fold(k, start):
        def rows(i, carry):
            here = pl.ds(pl.multiple_of(start + i * 16, 16), 16)
            h0[here, main_cols] = h0[here, main_cols] + hf[k, here, :].astype(F32)
            return carry

        lax.fori_loop(0, (512 - TOP if start else TOP) // 16, rows, 0)

    def finish(k, start):
        def rows(i, carry):
            here = pl.ds(pl.multiple_of(start + i * 16, 16), 16)
            total = h0[here, main_cols] + hf[k, here, :].astype(F32)
            h0[here, main_cols] = total * slope_v[here, main_cols]
            return carry

        lax.fori_loop(0, (512 - TOP if start else TOP) // 16, rows, 0)

    own_first(2)
    gelu(0)
    gelu(3)
    to_others()
    act_own(0)
    side_own()
    gelu(2)
    own_first(3)
    gelu(1)
    weight_hop(1)
    own_twin(0, t)
    own_hop(1)
    own_hop(2)
    own_hop(0)
    got_seg.wait()
    got_qkv.wait()
    attend(3)
    side_hop(1)
    act_own(1)
    own_hop(3)
    attend(1)
    attend(0)
    act_own(2)
    other_first(3)
    attend(2)
    own_twin(1, t_left)
    weight_hop(2)
    other_first(2)
    got_ow.wait()
    lax.fori_loop(0, 1, project, 0)
    act_own(3)
    own_far()
    other_first(1)
    own_twin(2, t_right)
    lax.fori_loop(1, 2, project, 0)
    own_twin(3, t_far)
    lax.fori_loop(2, 6, project, 0)
    own_all()
    lax.fori_loop(6, 7, project, 0)
    for e in range(4):
        side_part(e)
    side_send(0, 0, 0, False)
    side_send(1, 0, 1, False)
    side_send(0, 1, 1, False)
    side_send(1, 1, 0, False)
    other_hop(3)
    other_twin(0, t)
    lax.fori_loop(7, 8, project, 0)
    weight_part(0, True)
    other_hop(2)
    act_hop(0)
    other_hop(1)
    act_hop(1)
    for e in (2, 1, 3, 0):
        send(ATS + e, att_p.at[xx[e], oc], att_r.at[xx[e]], c=oc)
    weight_hop(3)
    other_twin(1, t_left)
    act_hop(2)
    side_send(0, 1, 0, True)
    side_send(1, 1, 1, True)
    act_hop(3)
    att_first()
    other_twin(2, t_right)
    side_hop(2)
    side_send(0, 2, 1, True)
    side_send(1, 2, 0, True)
    other_far()
    other_twin(3, t_far)
    weight_far()
    other_all()
    hidden(2, to_send(2))
    send(HHS, hp.at[1, top], hh.at[0, hh_rows[0]], y=yy[1])
    send(HHS + 1, hp.at[1, bottom], hh.at[1, hh_rows[1]], y=yy[3])
    side_send(0, 2, 0, True)
    side_send(1, 2, 1, True)
    weight_part(3, False)
    weight_part(1, False)
    act_far()
    side_hop(3)
    weight_tile(2, 0)
    grad_send(0, 0, 0, False)
    grad_send(1, 0, 1, False)
    hidden(3, to_send(3))
    send(HFS + 1, hp.at[2, top], hf.at[1, top], y=yy[3])
    side_send(0, 3, 1, True)
    side_send(1, 3, 0, True)
    hidden(1, to_send(1))
    send(HFS, hp.at[0, bottom], hf.at[0, bottom], y=yy[1])
    lax.fori_loop(1, 4, lambda i, carry: weight_tile(2, i), None)
    side_far()
    att_second()
    side_send(0, 3, 0, True)
    side_send(1, 3, 1, True)
    grad_send(0, 1, 1, False)
    grad_send(1, 1, 0, False)
    grad_send(0, 1, 0, True)
    grad_send(1, 1, 1, True)
    side_sum()
    hidden_hop(0)
    hidden_hop(1)
    hidden(0, to_keep)
    grad_send(0, 2, 1, True)
    grad_send(1, 2, 0, True)
    grad_send(0, 2, 0, True)
    grad_send(1, 2, 1, True)
    arrived(HFS, hf.at[0, bottom], y=yy[3])
    fold(0, TOP)
    arrived(HFS + 1, hf.at[1, top], y=yy[1])
    fold(1, 0)
    side_last()
    grad_send(0, 3, 1, True)
    grad_send(1, 3, 0, True)
    hidden_side()
    grad_send(0, 3, 0, True)
    grad_send(1, 3, 1, True)
    att_last()

    def grad_last(half):
        here = pl.ds(half * 64, 64)
        for k in range(2):
            arrived(grad_id(k, 3, half), gr.at[k, 3, here], z=zz[7] if k == 0 else zz[1])
        total = acc[z, here, :] + gr[0, 3, here, :].astype(F32) + gr[1, 3, here, :].astype(F32)
        go[here, act_cols] = total * (1.0 / 32.0)

    grad_last(0)
    grad_last(1)
    arrived(HFS + 2, hf.at[0, top], y=yy[3])
    finish(0, 0)
    arrived(HFS + 3, hf.at[1, bottom], y=yy[1])
    finish(1, TOP)

    for copy in sent[-N_SEND:]:
        copy.wait_send()
    assert len(place) == N_IDS, len(place)


def put(a, b, c, a_out, b_out, c_out, sem):
    copies = []
    pieces = [(b, b_out, i * 128, 128) for i in range(4)] + [(a, a_out, i * 16, 16) for i in range(4)]
    for k, (src, dst, start, rows) in enumerate(pieces + [(c, c_out, 0, 128)]):
        here = pl.ds(start, rows)
        copies.append(pltpu.make_async_copy(src.at[here], dst.at[here], sem.at[k]))
        copies[-1].start()
    for copy in copies:
        copy.wait()


def body(*args):
    hbm = pl.BlockSpec(memory_space=pltpu.HBM)
    vmem = pltpu.VMEM
    in_vmem = (pl.BlockSpec(memory_space=pltpu.VMEM),) * 3
    shapes = (
        jax.ShapeDtypeStruct((64, 4096), F32),
        jax.ShapeDtypeStruct((512, 1024), F32),
        jax.ShapeDtypeStruct((128, 1024), F32),
    )
    parts = pl.pallas_call(
        kernel,
        out_shape=shapes,
        in_specs=[hbm] * 7,
        out_specs=in_vmem,
        scratch_shapes=[
            vmem((3, 512, 512), BF),
            vmem((1, 8, 64), jnp.int32),
            vmem((4096, 512), BF),
            vmem((4096,), BF),
            vmem((512, 1024), BF),
            vmem((512, 1024), F32),
            vmem((4, 8, 64, 1024), BF),
            vmem((3, 8, 64, 1024), BF),
            vmem((8, 128, 1024), BF),
            vmem((3, 8, 128, CO), BF),
            vmem((4, 512, 1024), BF),
            vmem((512, 512), BF),
            vmem((4, 2, 64, 4096), BF),
            vmem((4, 64, 4096), BF),
            vmem((2, 64, 2048), BF),
            vmem((2, 64, 4096), BF),
            vmem((3, 512, CQ), BF),
            vmem((2, max(TOP, 512 - TOP), CQ), BF),
            vmem((2, 512, CQ), BF),
            vmem((8, 128, CA), F32),
            vmem((2, 4, 128, CA), BF),
            vmem((2, 4, 128, CA), BF),
            vmem((8, 4, CW, 128), BF),
            vmem((2, 4, 4, CW, 128), BF),
            vmem((3, CW, 128), BF),
            pltpu.SemaphoreType.DMA((N_SEND,)),
            pltpu.SemaphoreType.DMA((N_IDS,)),
            pltpu.SemaphoreType.DMA((N_LOCAL,)),
        ],
        compiler_params=pltpu.CompilerParams(
            collective_id=0, has_side_effects=True, vmem_limit_bytes=50 * 1024 * 1024
        ),
        name="layer",
    )(*(pltpu.with_memory_space_constraint(a, pltpu.HBM) for a in args))
    return pl.pallas_call(
        put,
        out_shape=shapes,
        in_specs=in_vmem,
        out_specs=(hbm,) * 3,
        scratch_shapes=[pltpu.SemaphoreType.DMA((9,))],
        compiler_params=pltpu.CompilerParams(vmem_limit_bytes=1 * 1024 * 1024),
        name="put",
    )(*parts)


def solution(mesh):
    finer = Mesh(mesh.devices.reshape(4, 8, 4, 2), ("y", "z", "x", "c"))
    tensor = ("x", "c")
    in_specs = (
        P(None, DP, tensor),
        P(DP, None, None),
        P(None, tensor),
        P(),
        P(DP_TENSOR, None),
        P(DP, tensor),
        P(DP, tensor),
    )
    out_specs = (P(DP_TENSOR, None), P(DP, tensor), P(DP, tensor))
    return jax.shard_map(body, mesh=finer, in_specs=in_specs, out_specs=out_specs, check_vma=False)
```
